512 devices in a mesh: row: 16 (over z), col: 32 (over x, y, core).
Axes of the slice: x: 4, y: 4, z: 16, core: 2. Of those that a mesh axis runs over, the one named last changes fastest.
Arguments:
- train_points: float32 [16, 32, 16384], P('row', None, 'col'), as said below
- targets: float32 [16, 16384], P('row', 'col'), may hold values from -16 to 16
- inverse_factor: float32 [16, 16384, 1024], P('row', 'col'), as said below
- counts: int32 [16, 16], P('row'), may hold values from 512 to 1024, as said below
- membership: int32 [16, 16, 64], replicated, may hold values from 0 to 1, as said below
- test_points: float32 [64, 32, 128], P('row'), may hold values from -6 to 6
Outputs:
- pred_mean: float32 [64, 128], P('row')
- pred_var: float32 [64, 128], P('row')
The draws below stay inside these ranges and needn't reach their ends.
Inputs may be any that keep to these rules, and one draw needn't show every extreme that they name: Each expert membership[r, c, :] takes part in at least one and at most 8 blocks, exactly 8 for at least one expert, and in at most one of the 4 blocks of each owner row. `counts`: at least one expert has all 1024 points valid. `inverse_factor`: F[i, j] as in the reference program is entry (i, j) of the inverse of the lower Cholesky factor of the expert's matrix whose entries are exp(-|x_i - x_j|^2 / 32), plus 0.1 on the diagonal, for valid i and j, and that is the identity elsewhere. `train_points`: each expert's 1024 points are drawn independently of the other experts' points.
All inputs are finite; a program needn't handle non-finite values.
Results may differ from the reference program's by a relative error of at most 0.0003.
Values sent between devices are 32-bit elements; how exact they have to be, the bound alone decides.
No kernel may reach another device: no remote copies, remote signals or barrier semaphores. Data moves between devices by JAX's collectives and lax.ppermute only.
A program may use at most 64 MiB of HBM per device.

```python
import jax
import jax.numpy as jnp
from jax import lax

D = 32
N_PTS = 1024
BS = 128
BPR = 4
MAXB = 8
ECOL = 16
NBLK = 64
N_ROW = 16


SIGNAL = 1.0


NOISE = 0.1


def expert_points(key):
    experts_all = N_ROW * ECOL
    point_key = jax.random.fold_in(key, 11)
    points = jax.random.normal(point_key, (experts_all, N_PTS, D), jnp.float32)
    return points


def expert_counts(key):
    experts_all = N_ROW * ECOL
    drawn = jax.random.randint(jax.random.fold_in(key, 21), (experts_all,), N_PTS // 2, N_PTS + 1, jnp.int32)
    fullest = jax.random.randint(jax.random.fold_in(key, 22), (), 0, experts_all, jnp.int32)
    return drawn.at[fullest].set(N_PTS)


def factor_one(points, valid_count):
    row_valid = jnp.arange(N_PTS, dtype=jnp.int32) < valid_count
    squares = jnp.sum(points * points, axis=1)
    products = jnp.dot(points, points.T, precision=lax.Precision.HIGHEST)
    spread = squares[:, None] + squares[None, :] - 2.0 * products
    kernel = SIGNAL * jnp.exp(-spread / D)
    both_valid = row_valid[:, None] & row_valid[None, :]
    diagonal = jnp.where(row_valid, NOISE, 1.0).astype(jnp.float32)
    matrix = jnp.where(both_valid, kernel, 0.0) + jnp.diag(diagonal)
    lower = jnp.linalg.cholesky(matrix)
    identity = jnp.eye(N_PTS, dtype=jnp.float32)
    return lax.linalg.triangular_solve(lower, identity, left_side=True, lower=True)


def draw_train_points(key, part):
    experts_all = N_ROW * ECOL
    points = expert_points(key)
    stored = points.reshape(experts_all, N_PTS // 2, 2, D).transpose(0, 2, 1, 3).reshape(experts_all, N_PTS, D)
    return stored.reshape(N_ROW, ECOL, N_PTS, D).transpose(0, 3, 1, 2).reshape(N_ROW, D, ECOL * N_PTS)


def draw_inverse_factor(key, part):
    experts_all = N_ROW * ECOL
    points = expert_points(key)
    valid_counts = expert_counts(key)
    factors = lax.map(lambda expert_items: factor_one(expert_items[0], expert_items[1]), (points, valid_counts))
    stored = factors.reshape(experts_all, N_PTS // 2, 2, N_PTS).transpose(0, 2, 1, 3)
    return stored.reshape(N_ROW, ECOL * N_PTS, N_PTS)


def draw_counts(key, part):
    return expert_counts(key).reshape(N_ROW, ECOL)


def draw_membership(key, part):
    experts_all = N_ROW * ECOL
    base_key = jax.random.fold_in(key, 31)
    is_busy = jax.random.randint(jax.random.fold_in(base_key, 1), (experts_all,), 0, 8, jnp.int32) == 0
    light = jax.random.randint(jax.random.fold_in(base_key, 2), (experts_all,), 1, MAXB // 2 + 1, jnp.int32)
    taken = jnp.where(is_busy, MAXB, light).astype(jnp.int32)
    fullest = jax.random.randint(jax.random.fold_in(base_key, 3), (), 0, experts_all, jnp.int32)
    taken = taken.at[fullest].set(MAXB)
    expert_keys = jax.random.split(jax.random.fold_in(base_key, 4), experts_all)
    orders = jax.vmap(lambda one_key: jax.random.permutation(one_key, N_ROW))(expert_keys)
    places = jnp.argsort(orders, axis=1).astype(jnp.int32)
    chosen_rows = places < taken[:, None]
    block_picks = jax.random.randint(jax.random.fold_in(base_key, 5), (experts_all, N_ROW), 0, BPR, jnp.int32)
    inside = block_picks[:, :, None] == jnp.arange(BPR, dtype=jnp.int32)[None, None, :]
    member = chosen_rows[:, :, None] & inside
    return member.reshape(N_ROW, ECOL, N_ROW * BPR).astype(jnp.int32)


def block_scale(stream_key, dims, cuts, least, top_value):
    def one(axis_at, parts):
        heights = jax.random.uniform(jax.random.fold_in(jax.random.fold_in(stream_key, 6), axis_at), (parts,), jnp.float32, least / len(cuts), top_value / len(cuts))
        return jnp.repeat(jnp.exp(heights), dims[axis_at] // parts).reshape((-1,) + (1,) * (len(dims) - axis_at - 1))

    loudness = one(*cuts[0])
    for cut in cuts[1:]:
        loudness = loudness * one(*cut)
    return loudness


def bell_draw(rng, dims, deviation, limit, shards=(), kind=jnp.bfloat16):
    gain = block_scale(rng, dims, shards, -0.22, 0.18) if shards else 1.0
    values = jax.random.normal(rng, dims, jnp.float32) * deviation * gain
    return jnp.minimum(jnp.maximum(values, -limit), limit).astype(kind)


def setup_inputs(seed: int = 0) -> dict:
    streams_of = jax.random.split(jax.random.key(seed), 7)
    return {
        "train_points": draw_train_points(jax.random.fold_in(streams_of[6], 71), 0),
        "targets": bell_draw(streams_of[1], (N_ROW, ECOL * N_PTS), 3.0, 16.0, ((0, 16), (1, 32)), jnp.float32),
        "inverse_factor": draw_inverse_factor(jax.random.fold_in(streams_of[6], 71), 0),
        "counts": draw_counts(jax.random.fold_in(streams_of[6], 71), 0),
        "membership": draw_membership(jax.random.fold_in(streams_of[6], 71), 0),
        "test_points": bell_draw(streams_of[5], (NBLK, D, BS), 1.0, 6.0, ((0, 16),), jnp.float32),
    }


SIGNAL = 1.0
NOISE = 0.1
HIGHEST = lax.Precision.HIGHEST

def cross_kernel(train_cols, test_cols, squared_scale):
    products = jnp.einsum('dn,dp->np', train_cols, test_cols, precision=HIGHEST)
    spread = jnp.sum(train_cols * train_cols, axis=0)[:, None] + jnp.sum(test_cols * test_cols, axis=0)[None, :] - 2.0 * products
    return SIGNAL * jnp.exp(-0.5 * spread / squared_scale)

def slot_table(member, slot_count):
    member_flags = member.astype(jnp.int32)
    before = jnp.cumsum(member_flags) - member_flags
    slot_ids = jnp.arange(slot_count, dtype=jnp.int32)[:, None]
    picked = ((member_flags[None, :] == 1) & (before[None, :] == slot_ids)).astype(jnp.int32)
    chosen = jnp.sum(picked * jnp.arange(member.shape[0], dtype=jnp.int32)[None, :], axis=1).astype(jnp.int32)
    return (picked.astype(jnp.float32), chosen)

def weigh_expert(mean_part, quad_part):
    variance = NOISE + jnp.maximum(SIGNAL - quad_part, 0.0)
    entropy_gap = 0.5 * (jnp.log(SIGNAL + NOISE) - jnp.log(variance))
    weight = entropy_gap / variance
    return (weight * mean_part, weight)

def reference(train_points, targets, inverse_factor, counts, membership, test_points):
    features = train_points.shape[1]
    squared_scale = 0.5 * features
    experts_all = N_ROW * ECOL
    half_pts = N_PTS // 2
    train_all = train_points.reshape(N_ROW, features, ECOL, N_PTS).transpose(0, 2, 1, 3).reshape(experts_all, features, 2, half_pts)
    train_all = train_all.transpose(0, 1, 3, 2).reshape(experts_all, features, N_PTS)
    target_all = targets.reshape(experts_all, 2, half_pts).transpose(0, 2, 1).reshape(experts_all, N_PTS)
    factor_all = inverse_factor.reshape(experts_all, 2, half_pts, N_PTS).transpose(0, 2, 1, 3).reshape(experts_all, N_PTS, N_PTS)
    count_all = counts.reshape(experts_all)
    member_all = membership.reshape(experts_all, NBLK)

    def accumulate(totals, expert_items):
        train_cols, target_col, factor, valid_count, member = expert_items
        picked, chosen = slot_table(member, MAXB)
        test_cols = test_points[chosen].transpose(1, 0, 2).reshape(features, MAXB * BS)
        row_valid = jnp.arange(N_PTS, dtype=jnp.int32) < valid_count
        kernel = jnp.where(row_valid[:, None], cross_kernel(train_cols, test_cols, squared_scale), 0.0)
        solved = jnp.dot(factor.astype(jnp.float32), kernel.astype(jnp.float32), precision=HIGHEST, preferred_element_type=jnp.float32)
        whitened = jnp.dot(factor.astype(jnp.float32), target_col.astype(jnp.float32), precision=HIGHEST, preferred_element_type=jnp.float32)
        mean_part = jnp.dot(whitened.astype(jnp.float32), solved.astype(jnp.float32), precision=HIGHEST, preferred_element_type=jnp.float32)
        quad_part = jnp.sum(solved * solved, axis=0)
        weighted, weight = weigh_expert(mean_part, quad_part)
        dense_num = jnp.einsum('sb,sp->bp', picked, weighted.reshape(MAXB, BS), precision=HIGHEST)
        dense_wgt = jnp.einsum('sb,sp->bp', picked, weight.reshape(MAXB, BS), precision=HIGHEST)
        return ((totals[0] + dense_num, totals[1] + dense_wgt), None)
    start = (jnp.zeros((NBLK, BS), jnp.float32), jnp.zeros((NBLK, BS), jnp.float32))
    totals, _ = lax.scan(accumulate, start, (train_all, target_all, factor_all, count_all, member_all))
    precision_sum = 1.0 / (SIGNAL + NOISE) + totals[1]
    return (totals[0] / precision_sum, 1.0 / precision_sum)
```

```python
import math

import jax
import jax.numpy as jnp
from jax import lax
from jax.experimental import pallas as pl
from jax.experimental.pallas import tpu as pltpu
from jax.sharding import PartitionSpec as P

SIGNAL = 1.0
NOISE = 0.1
BF16 = jnp.bfloat16
F32 = jnp.float32
I32 = jnp.int32
LANES = 128
SUBLANES = 8


def three_parts(v):
    high = v.astype(BF16).astype(F32)
    rest = v - high
    mid = rest.astype(BF16).astype(F32)
    return high, mid, (rest - mid).astype(BF16).astype(F32)


def two_parts(v):
    high = v.astype(BF16)
    return high, (v - high.astype(F32)).astype(BF16)


def place():
    col = lax.axis_index("col")
    return lax.axis_index("row"), col // 2, col % 2


def send_kernel(member_hbm, tests_hbm, points_hbm, targets_hbm, out_ref, packed_ref, wanted_ref,
                member_ref, tests_ref, sems):
    own_row, expert, _ = place()
    peers = member_hbm.shape[0]
    blocks_own, features, _ = tests_hbm.shape
    near = pl.multiple_of(expert // SUBLANES * SUBLANES, SUBLANES)
    copies = [
        pltpu.make_async_copy(member_hbm.at[:, pl.ds(near, SUBLANES), :], member_ref, sems.at[0]),
        pltpu.make_async_copy(tests_hbm, tests_ref, sems.at[1]),
        pltpu.make_async_copy(points_hbm.at[0], packed_ref.at[0:features], sems.at[2]),
        pltpu.make_async_copy(targets_hbm, packed_ref.at[features : features + 1], sems.at[3]),
    ]
    for c in copies:
        c.start()
    copies[0].wait()
    member = member_ref[...].astype(F32)
    sub = lax.broadcasted_iota(I32, member.shape, 1)
    mine = jnp.sum(jnp.where(sub == expert - near, member, 0.0), axis=1)
    lane = lax.broadcasted_iota(I32, mine.shape, 1)
    wanted = [
        jnp.sum(jnp.where(lane == own_row * blocks_own + b, mine, 0.0), axis=1, keepdims=True)
        for b in range(blocks_own)
    ]
    wide = [jnp.broadcast_to(w, (peers, LANES)) for w in wanted]
    for b in range(blocks_own):
        wanted_ref[b] = wide[b]
    copies[1].wait()
    blocks = [tests_ref[b] for b in range(blocks_own)]
    for r in range(peers):
        total = blocks[0] * wide[0][r : r + 1]
        for b in range(1, blocks_own):
            total = total + blocks[b] * wide[b][r : r + 1]
        out_ref[r] = total
    copies[2].wait()
    copies[3].wait()


def prepare_kernel(member_hbm, counts_hbm, own_f_hbm, own_ref, other_ref, other_f_ref,
                   aug_ref, fh_ref, fl_hbm, alpha_ref, slots_ref,
                   member_ref, counts_ref, own_f_ref, fl_ref, *rest, scale, step):
    cols_refs, sems = rest[:-1], rest[-1]
    own_row, expert, parity = place()
    half = own_ref.shape[1]
    features = scale[1]
    factor = scale[0]
    near = pl.multiple_of(expert // SUBLANES * SUBLANES, SUBLANES)
    chunks = half // step
    small = [
        pltpu.make_async_copy(counts_hbm, counts_ref, sems.at[0]),
        pltpu.make_async_copy(member_hbm.at[own_row, pl.ds(near, SUBLANES), :], member_ref, sems.at[1]),
    ]
    large = [
        pltpu.make_async_copy(
            own_f_hbm.at[0, step * a : step * a + step, 0 : 2 * step * (a + 1)],
            own_f_ref.at[step * a : step * a + step, 0 : 2 * step * (a + 1)],
            sems.at[2 + a],
        )
        for a in range(chunks)
    ]
    for c in small + large:
        c.start()
    small[0].wait()
    counts = counts_ref[...]
    lane = lax.broadcasted_iota(I32, counts.shape, 1)
    valid = jnp.sum(jnp.where(lane == expert, counts, 0).astype(F32), axis=1, keepdims=True)

    def columns(ref, odd):
        points, y = ref[0:features, :], ref[features : features + 1, :]
        where = 2 * lax.broadcasted_iota(I32, (1, half), 1) + odd
        alive = where.astype(F32) < valid
        scaled = jnp.where(alive, points * (2.0 * factor), 0.0)
        square = jnp.where(alive, -factor * jnp.sum(points * points, axis=0, keepdims=True), -1e9)
        xh, xm, xl = three_parts(scaled)
        sh, sm, sl = three_parts(square)
        row = lax.broadcasted_iota(I32, (features, half), 0)
        last = jnp.where(row == 0, sh, jnp.where(row == 1, sm, jnp.where(row == 2, sl, 0.0)))
        last = jnp.where((row >= 3) & (row < 6), 1.0, last)
        wide = [xh, xh, xm, xm, xh, xl, last, jnp.zeros_like(xh), jnp.broadcast_to(y, (LANES, half))]
        return jnp.concatenate(wide, axis=0).T

    own = columns(own_ref, parity)
    other = columns(other_ref, 1 - parity)
    first = jnp.where(parity == 0, own, other)
    second = jnp.where(parity == 0, other, own)
    for c, ref in enumerate(cols_refs):
        at = slice(c * LANES, c * LANES + LANES)
        ref[pl.ds(0, half, 2), :] = first[:, at]
        ref[pl.ds(1, half, 2), :] = second[:, at]
    aug_ref[:, 0:LANES] = cols_refs[0][...].astype(BF16)
    aug_ref[:, LANES : 2 * LANES] = cols_refs[1][...].astype(BF16)
    yh, yl = two_parts(cols_refs[2][...])

    small[1].wait()
    member = member_ref[...].astype(F32)
    sub = lax.broadcasted_iota(I32, member.shape, 0)
    mine = jnp.sum(jnp.where(sub == expert - near, member, 0.0), axis=0, keepdims=True)
    peers = slots_ref.shape[1]
    blocks_own = mine.shape[1] // peers
    row = lax.broadcasted_iota(I32, (peers, mine.shape[1]), 0)
    lane = lax.broadcasted_iota(I32, (peers, mine.shape[1]), 1)
    inside = (lane >= row * blocks_own) & (lane < row * blocks_own + blocks_own)
    held = jnp.sum(jnp.where(inside, mine, 0.0), axis=1, keepdims=True)
    before = jnp.sum(jnp.where(lane < row * blocks_own, mine, 0.0), axis=1, keepdims=True)
    for m in range(slots_ref.shape[0]):
        taken = (before == (2 * m + parity).astype(F32)) & (held > 0.5)
        slots_ref[m] = jnp.broadcast_to(jnp.where(taken, 1.0, 0.0), (peers, LANES))

    leaving = []
    sums = [jnp.zeros((SUBLANES, LANES), F32) for _ in range(2 * half // LANES)]
    for which in (1, 0):
        for a in range(chunks):
            reach = 2 * step * (a + 1)
            if which == 0:
                large[a].wait()
            src = (own_f_ref, other_f_ref)[which]
            to = slice(2 * step * a + step * which, 2 * step * a + step * which + step)
            f = src[step * a : step * a + step, 0:reach]
            fh, fl = two_parts(f)
            fh_ref[to, 0:reach] = fh
            fl_ref[to, 0:reach] = fl
            leaving.append(pltpu.make_async_copy(fl_ref.at[to, 0:reach], fl_hbm.at[to, 0:reach], sems.at[2 + chunks + len(leaving)]))
            leaving[-1].start()
            w = jnp.dot(fh, yh[0:reach], preferred_element_type=F32)
            w = w + jnp.dot(fh, yl[0:reach], preferred_element_type=F32)
            w = w + jnp.dot(fl, yh[0:reach], preferred_element_type=F32)
            for c in range(reach // LANES):
                part = f[:, c * LANES : c * LANES + LANES] * w
                sums[c] = sums[c] + jnp.sum(part.reshape(step // SUBLANES, SUBLANES, LANES), axis=0)
    for c, part in enumerate(sums):
        alpha = jnp.broadcast_to(jnp.sum(part, axis=0, keepdims=True), (LANES, LANES))
        alpha_ref[c * LANES : c * LANES + LANES, :] = alpha.T
    for c in leaving:
        c.wait()


def expert_kernel(aug_ref, fh_ref, fl_hbm, alpha_ref, slots_ref, tests_ref, out_ref, kh_ref, kl_ref, fl_ref, sems, *, scale, step):
    points = aug_ref.shape[0]
    coming = [
        pltpu.make_async_copy(
            fl_hbm.at[step * a : step * a + step, 0 : step * (a + 1)],
            fl_ref.at[step * a : step * a + step, 0 : step * (a + 1)],
            sems.at[a],
        )
        for a in range(points // step)
    ]
    for c in coming:
        c.start()
    slots, peers, _ = slots_ref.shape
    _, features, block = tests_ref.shape
    width = slots * block
    chosen = []
    for m in range(slots):
        s = slots_ref[m]
        total = tests_ref[0] * s[0:1]
        for r in range(1, peers):
            total = total + tests_ref[r] * s[r : r + 1]
        chosen.append(total)
    t = jnp.concatenate(chosen, axis=1)
    th, tm, tl = three_parts(t)
    square = -scale * jnp.sum(t * t, axis=0, keepdims=True)
    sh, sm, sl = three_parts(square)
    row = lax.broadcasted_iota(I32, (features, width), 0)
    last = jnp.where(row == 3, sh, jnp.where(row == 4, sm, jnp.where(row == 5, sl, 0.0)))
    last = jnp.where(row < 3, 1.0, last)
    taug = jnp.concatenate([th, tm, th, tm, tl, th, last, jnp.zeros_like(th)], axis=0).astype(BF16)
    quad = jnp.zeros((1, width), F32)
    mean = jnp.zeros((1, width), F32)
    for a in range(points // step):
        at = slice(a * step, a * step + step)
        k = jnp.exp2(jnp.dot(aug_ref[at, :], taug, preferred_element_type=F32))
        kh, kl = two_parts(k)
        kh_ref[at, :] = kh
        kl_ref[at, :] = kl
        mean = mean + jnp.sum(k * jnp.concatenate([alpha_ref[at, :]] * slots, axis=1), axis=0, keepdims=True)
    for a in range(points // step):
        at = slice(a * step, a * step + step)
        reach = step * (a + 1)
        solved = jnp.dot(fh_ref[at, 0:reach], kh_ref[0:reach, :], preferred_element_type=F32)
        coming[a].wait()
        solved = solved + jnp.dot(fl_ref[at, 0:reach], kh_ref[0:reach, :], preferred_element_type=F32)
        solved = solved + jnp.dot(fh_ref[at, 0:reach], kl_ref[0:reach, :], preferred_element_type=F32)
        quad = quad + jnp.sum(solved * solved, axis=0, keepdims=True)
    variance = NOISE + jnp.maximum(SIGNAL - quad, 0.0)
    gap = 0.5 * (math.log(SIGNAL + NOISE) - jnp.log(variance))
    weight = gap / variance
    both = jnp.concatenate([weight * mean, weight], axis=0)
    for r in range(peers):
        total = both[:, 0:block] * slots_ref[0, r : r + 1]
        for m in range(1, slots):
            total = total + both[:, m * block : m * block + block] * slots_ref[m, r : r + 1]
        out_ref[r] = total


def owner_kernel(wanted_ref, parts_ref, out_ref):
    peers, _, _ = parts_ref.shape
    blocks = wanted_ref.shape[0]
    num, wgt = [], []
    for b in range(blocks):
        total = parts_ref[0] * wanted_ref[b, 0:1]
        for r in range(1, peers):
            total = total + parts_ref[r] * wanted_ref[b, r : r + 1]
        num.append(total[0:1])
        wgt.append(total[1:2])
    tile = jnp.concatenate(num + wgt, axis=0)
    for j in range(out_ref.shape[0]):
        out_ref[j] = tile


def final_kernel(parts_ref, mean_ref, var_ref):
    parts = [parts_ref[j] for j in range(parts_ref.shape[0])]
    while len(parts) > 1:
        parts = [parts[i] + parts[i + 1] for i in range(0, len(parts), 2)]
    total = parts[0]
    blocks = mean_ref.shape[0]
    precision = 1.0 / (SIGNAL + NOISE) + total[blocks:]
    mean_ref[...] = total[0:blocks] / precision
    var_ref[...] = 1.0 / precision


def hbm(x):
    return pltpu.with_memory_space_constraint(x, pltpu.HBM)


def vmem(x):
    return pltpu.with_memory_space_constraint(x, pltpu.VMEM)


def on_device(train_points, targets, inverse_factor, counts, membership, test_points):
    cols = lax.axis_size("col")
    rows = lax.axis_size("row")
    slots = min(8, rows) // 2
    blocks_own, features, block = test_points.shape
    half = train_points.shape[2]
    points = 2 * half
    scale = math.log2(math.e) / features
    swap = [(i, i ^ 1) for i in range(cols)]
    step = 128
    in_hbm = pl.BlockSpec(memory_space=pltpu.HBM)
    in_vmem = pl.BlockSpec(memory_space=pltpu.VMEM)
    held = features + SUBLANES

    outgoing, packed, wanted = pl.pallas_call(
        send_kernel,
        out_shape=(pltpu.VMEM((rows, features, block), F32), pltpu.VMEM((held, half), F32), pltpu.VMEM((blocks_own, rows, LANES), F32)),
        in_specs=[in_hbm] * 4,
        out_specs=(in_vmem,) * 3,
        scratch_shapes=[pltpu.VMEM((rows, SUBLANES, membership.shape[2]), I32), pltpu.VMEM((blocks_own, features, block), F32), pltpu.SemaphoreType.DMA((4,))],
        compiler_params=pltpu.CompilerParams(vmem_limit_bytes=4 << 20),
        name="send",
    )(hbm(membership), hbm(test_points), hbm(train_points), hbm(targets))
    tests = lax.all_to_all(outgoing, "row", split_axis=0, concat_axis=0, tiled=True)
    other_factor = lax.ppermute(inverse_factor[0], "col", swap)
    other = lax.ppermute(packed, "col", swap)

    aug, fh, fl, alpha, table = pl.pallas_call(
        lambda *refs: prepare_kernel(*refs, scale=(scale, features), step=step),
        out_shape=(
            pltpu.VMEM((points, 2 * LANES), BF16),
            pltpu.VMEM((points, points), BF16),
            pltpu.HBM((points, points), BF16),
            pltpu.VMEM((points, LANES), F32),
            pltpu.VMEM((slots, rows, LANES), F32),
        ),
        in_specs=[in_hbm] * 3 + [in_vmem] * 3,
        out_specs=(in_vmem, in_vmem, in_hbm, in_vmem, in_vmem),
        scratch_shapes=[
            pltpu.VMEM((SUBLANES, membership.shape[2]), I32),
            pltpu.VMEM(counts.shape, I32),
            pltpu.VMEM((half, points), F32),
            pltpu.VMEM((points, points), BF16),
            pltpu.VMEM((points, LANES), F32),
            pltpu.VMEM((points, LANES), F32),
            pltpu.VMEM((points, LANES), F32),
            pltpu.SemaphoreType.DMA((2 + 3 * (half // step),)),
        ],
        compiler_params=pltpu.CompilerParams(vmem_limit_bytes=20 << 20),
        name="prepare",
    )(hbm(membership), hbm(counts), hbm(inverse_factor), vmem(packed), vmem(other), vmem(other_factor))
    parts = pl.pallas_call(
        lambda *refs: expert_kernel(*refs, scale=scale, step=2 * step),
        out_shape=pltpu.VMEM((rows, 2, block), F32),
        in_specs=[in_vmem] * 2 + [in_hbm] + [in_vmem] * 3,
        out_specs=in_vmem,
        scratch_shapes=[pltpu.VMEM((points, slots * block), BF16)] * 2 + [pltpu.VMEM((points, points), BF16), pltpu.SemaphoreType.DMA((half // step,))],
        compiler_params=pltpu.CompilerParams(vmem_limit_bytes=16 << 20),
        name="expert",
    )(vmem(aug), vmem(fh), hbm(fl), vmem(alpha), vmem(table), vmem(tests))
    arrived = lax.all_to_all(parts, "row", split_axis=0, concat_axis=0, tiled=True)
    spread = pl.pallas_call(
        owner_kernel,
        out_shape=pltpu.VMEM((cols, 2 * blocks_own, block), F32),
        in_specs=[in_vmem] * 2,
        out_specs=in_vmem,
        compiler_params=pltpu.CompilerParams(vmem_limit_bytes=4 << 20),
        name="owner",
    )(vmem(wanted), vmem(arrived))
    shares = lax.all_to_all(spread, "col", split_axis=0, concat_axis=0, tiled=True)
    return pl.pallas_call(
        final_kernel,
        out_shape=(jax.ShapeDtypeStruct((blocks_own, block), F32),) * 2,
        in_specs=[in_vmem],
        out_specs=(in_vmem,) * 2,
        compiler_params=pltpu.CompilerParams(vmem_limit_bytes=4 << 20),
        name="final",
    )(vmem(shares))


def solution(mesh):
    in_specs = (
        P("row", None, "col"),
        P("row", "col"),
        P("row", "col", None),
        P("row", None),
        P(),
        P("row", None, None),
    )
    out_specs = (P("row", None), P("row", None))

    return jax.shard_map(on_device, mesh=mesh, in_specs=in_specs, out_specs=out_specs, check_vma=False)
```

```python
import math

import jax
import jax.numpy as jnp
from jax import lax
from jax.experimental import pallas as pl
from jax.experimental.pallas import tpu as pltpu
from jax.sharding import PartitionSpec as P

SIGNAL = 1.0
NOISE = 0.1
BF16 = jnp.bfloat16
F32 = jnp.float32
I32 = jnp.int32
LANES = 128
SUBLANES = 8


def three_parts(v):
    high = v.astype(BF16).astype(F32)
    rest = v - high
    mid = rest.astype(BF16).astype(F32)
    return high, mid, (rest - mid).astype(BF16).astype(F32)


def two_parts(v):
    high = v.astype(BF16)
    return high, (v - high.astype(F32)).astype(BF16)


def place():
    col = lax.axis_index("col")
    return lax.axis_index("row"), col // 2, col % 2


def send_kernel(member_hbm, tests_hbm, points_hbm, targets_hbm, out_ref, packed_ref, wanted_ref,
                member_ref, tests_ref, sems):
    own_row, expert, _ = place()
    peers = member_hbm.shape[0]
    blocks_own, features, _ = tests_hbm.shape
    near = pl.multiple_of(expert // SUBLANES * SUBLANES, SUBLANES)
    copies = [
        pltpu.make_async_copy(member_hbm.at[:, pl.ds(near, SUBLANES), :], member_ref, sems.at[0]),
        pltpu.make_async_copy(tests_hbm, tests_ref, sems.at[1]),
        pltpu.make_async_copy(points_hbm.at[0], packed_ref.at[0:features], sems.at[2]),
        pltpu.make_async_copy(targets_hbm, packed_ref.at[features : features + 1], sems.at[3]),
    ]
    for c in copies:
        c.start()
    copies[0].wait()
    member = member_ref[...].astype(F32)
    sub = lax.broadcasted_iota(I32, member.shape, 1)
    mine = jnp.sum(jnp.where(sub == expert - near, member, 0.0), axis=1)
    lane = lax.broadcasted_iota(I32, mine.shape, 1)
    wanted = [
        jnp.sum(jnp.where(lane == own_row * blocks_own + b, mine, 0.0), axis=1, keepdims=True)
        for b in range(blocks_own)
    ]
    wide = [jnp.broadcast_to(w, (peers, LANES)) for w in wanted]
    for b in range(blocks_own):
        wanted_ref[b] = wide[b]
    copies[1].wait()
    blocks = [tests_ref[b] for b in range(blocks_own)]
    for r in range(peers):
        total = blocks[0] * wide[0][r : r + 1]
        for b in range(1, blocks_own):
            total = total + blocks[b] * wide[b][r : r + 1]
        out_ref[r] = total
    copies[2].wait()
    copies[3].wait()


def first_column(a, step):
    return step * a * (a + 1)


def points_kernel(member_hbm, counts_hbm, own_ref, other_ref, aug_ref, y_ref, slots_ref,
                  member_ref, counts_ref, first_ref, second_ref, third_ref, sems, *, features, factor):
    own_row, expert, parity = place()
    half = own_ref.shape[1]
    near = pl.multiple_of(expert // SUBLANES * SUBLANES, SUBLANES)
    copies = [
        pltpu.make_async_copy(counts_hbm, counts_ref, sems.at[0]),
        pltpu.make_async_copy(member_hbm.at[own_row, pl.ds(near, SUBLANES), :], member_ref, sems.at[1]),
    ]
    for c in copies:
        c.start()
    for c in copies:
        c.wait()
    counts = counts_ref[...]
    lane = lax.broadcasted_iota(I32, counts.shape, 1)
    valid = jnp.sum(jnp.where(lane == expert, counts, 0).astype(F32), axis=1, keepdims=True)

    def columns(ref, odd):
        points, y = ref[0:features, :], ref[features : features + 1, :]
        where = 2 * lax.broadcasted_iota(I32, (1, half), 1) + odd
        alive = where.astype(F32) < valid
        scaled = jnp.where(alive, points * (2.0 * factor), 0.0)
        square = jnp.where(alive, -factor * jnp.sum(points * points, axis=0, keepdims=True), -1e9)
        xh, xm, xl = three_parts(scaled)
        sh, sm, sl = three_parts(square)
        row = lax.broadcasted_iota(I32, (features, half), 0)
        last = jnp.where(row == 0, sh, jnp.where(row == 1, sm, jnp.where(row == 2, sl, 0.0)))
        last = jnp.where((row >= 3) & (row < 6), 1.0, last)
        wide = [xh, xh, xm, xm, xh, xl, last, jnp.zeros_like(xh), jnp.broadcast_to(y, (LANES, half))]
        return jnp.concatenate(wide, axis=0)

    own = columns(own_ref, parity)
    other = columns(other_ref, 1 - parity)
    first = jnp.where(parity == 0, own, other)
    second = jnp.where(parity == 0, other, own)
    for c, ref in enumerate((first_ref, second_ref, third_ref)):
        at = slice(c * LANES, c * LANES + LANES)
        ref[pl.ds(0, half, 2), :] = first[at].T
        ref[pl.ds(1, half, 2), :] = second[at].T
    aug_ref[:, 0:LANES] = first_ref[...].astype(BF16)
    aug_ref[:, LANES : 2 * LANES] = second_ref[...].astype(BF16)
    yh, yl = two_parts(third_ref[...])
    y_ref[0] = yh
    y_ref[1] = yl

    member = member_ref[...].astype(F32)
    sub = lax.broadcasted_iota(I32, member.shape, 0)
    mine = jnp.sum(jnp.where(sub == expert - near, member, 0.0), axis=0, keepdims=True)
    peers = slots_ref.shape[1]
    blocks_own = mine.shape[1] // peers
    row = lax.broadcasted_iota(I32, (peers, mine.shape[1]), 0)
    lane = lax.broadcasted_iota(I32, (peers, mine.shape[1]), 1)
    inside = (lane >= row * blocks_own) & (lane < row * blocks_own + blocks_own)
    held = jnp.sum(jnp.where(inside, mine, 0.0), axis=1, keepdims=True)
    before = jnp.sum(jnp.where(lane < row * blocks_own, mine, 0.0), axis=1, keepdims=True)
    for m in range(slots_ref.shape[0]):
        taken = (before == (2 * m + parity).astype(F32)) & (held > 0.5)
        slots_ref[m] = jnp.broadcast_to(jnp.where(taken, 1.0, 0.0), (peers, LANES))


def factor_kernel(own_f_hbm, other_f_ref, y_ref, fh_ref, fl_ref, alpha_ref, own_f_ref, sems, *, step):
    half = own_f_ref.shape[0]
    chunks = half // step
    coming = [
        pltpu.make_async_copy(
            own_f_hbm.at[0, step * a : step * a + step, 0 : 2 * step * (a + 1)],
            own_f_ref.at[step * a : step * a + step, 0 : 2 * step * (a + 1)],
            sems.at[a],
        )
        for a in range(chunks)
    ]
    for c in coming:
        c.start()
    sums = [jnp.zeros((SUBLANES, LANES), F32) for _ in range(2 * half // LANES)]
    for which in (1, 0):
        for a in range(chunks):
            reach = 2 * step * (a + 1)
            if which == 0:
                coming[a].wait()
            src = (own_f_ref, other_f_ref)[which]
            to = slice(step * which, step * which + step)
            at = slice(first_column(a, step), first_column(a, step) + reach)
            f = src[step * a : step * a + step, 0:reach]
            fh, fl = two_parts(f)
            fh_ref[to, at] = fh
            fl_ref[to, at] = fl
            w = jnp.dot(fh, y_ref[0, 0:reach], preferred_element_type=F32)
            w = w + jnp.dot(fh, y_ref[1, 0:reach], preferred_element_type=F32)
            w = w + jnp.dot(fl, y_ref[0, 0:reach], preferred_element_type=F32)
            for c in range(reach // LANES):
                part = f[:, c * LANES : c * LANES + LANES] * w
                sums[c] = sums[c] + jnp.sum(part.reshape(step // SUBLANES, SUBLANES, LANES), axis=0)
    for c, part in enumerate(sums):
        alpha_ref[:, c * LANES : c * LANES + LANES] = jnp.broadcast_to(jnp.sum(part, axis=0, keepdims=True), (SUBLANES, LANES))


def expert_kernel(aug_ref, fh_ref, fl_ref, alpha_ref, slots_ref, tests_ref, out_ref, kh_ref, kl_ref, *, scale, step):
    points = aug_ref.shape[0]
    slots, peers, _ = slots_ref.shape
    _, features, block = tests_ref.shape
    width = slots * block
    chosen = []
    for m in range(slots):
        s = slots_ref[m]
        total = tests_ref[0] * s[0:1]
        for r in range(1, peers):
            total = total + tests_ref[r] * s[r : r + 1]
        chosen.append(total)
    t = jnp.concatenate(chosen, axis=1)
    th, tm, tl = three_parts(t)
    square = -scale * jnp.sum(t * t, axis=0, keepdims=True)
    sh, sm, sl = three_parts(square)
    row = lax.broadcasted_iota(I32, (features, width), 0)
    last = jnp.where(row == 3, sh, jnp.where(row == 4, sm, jnp.where(row == 5, sl, 0.0)))
    last = jnp.where(row < 3, 1.0, last)
    taug = jnp.concatenate([th, tm, th, tm, tl, th, last, jnp.zeros_like(th)], axis=0).astype(BF16)
    quad = jnp.zeros((1, width), F32)
    mean = jnp.zeros((1, width), F32)
    for a in range(points // step):
        at = slice(a * step, a * step + step)
        k = jnp.exp2(jnp.dot(aug_ref[at, :], taug, preferred_element_type=F32))
        kh, kl = two_parts(k)
        kh_ref[at, :] = kh
        kl_ref[at, :] = kl
        alpha = jnp.concatenate(
            [
                jnp.broadcast_to(alpha_ref[0:1, c : c + LANES], (LANES, LANES)).T
                for c in range(a * step, a * step + step, LANES)
            ],
            axis=0,
        )
        mean = mean + jnp.sum(k * jnp.concatenate([alpha] * slots, axis=1), axis=0, keepdims=True)
    for a in range(points // step):
        reach = step * (a + 1)
        at = slice(first_column(a, step // 2), first_column(a, step // 2) + reach)
        solved = jnp.dot(fh_ref[:, at], kh_ref[0:reach, :], preferred_element_type=F32)
        solved = solved + jnp.dot(fl_ref[:, at], kh_ref[0:reach, :], preferred_element_type=F32)
        solved = solved + jnp.dot(fh_ref[:, at], kl_ref[0:reach, :], preferred_element_type=F32)
        quad = quad + jnp.sum(solved * solved, axis=0, keepdims=True)
    variance = NOISE + jnp.maximum(SIGNAL - quad, 0.0)
    gap = 0.5 * (math.log(SIGNAL + NOISE) - jnp.log(variance))
    weight = gap / variance
    both = jnp.concatenate([weight * mean, weight], axis=0)
    for r in range(peers):
        total = both[:, 0:block] * slots_ref[0, r : r + 1]
        for m in range(1, slots):
            total = total + both[:, m * block : m * block + block] * slots_ref[m, r : r + 1]
        out_ref[r] = total


def owner_kernel(wanted_ref, parts_ref, out_ref):
    peers, _, _ = parts_ref.shape
    blocks = wanted_ref.shape[0]
    num, wgt = [], []
    for b in range(blocks):
        total = parts_ref[0] * wanted_ref[b, 0:1]
        for r in range(1, peers):
            total = total + parts_ref[r] * wanted_ref[b, r : r + 1]
        num.append(total[0:1])
        wgt.append(total[1:2])
    tile = jnp.concatenate(num + wgt, axis=0)
    for j in range(out_ref.shape[0]):
        out_ref[j] = tile


def final_kernel(parts_ref, mean_ref, var_ref):
    parts = [parts_ref[j] for j in range(parts_ref.shape[0])]
    while len(parts) > 1:
        parts = [parts[i] + parts[i + 1] for i in range(0, len(parts), 2)]
    total = parts[0]
    blocks = mean_ref.shape[0]
    precision = 1.0 / (SIGNAL + NOISE) + total[blocks:]
    mean_ref[...] = total[0:blocks] / precision
    var_ref[...] = 1.0 / precision


def hbm(x):
    return pltpu.with_memory_space_constraint(x, pltpu.HBM)


def vmem(x):
    return pltpu.with_memory_space_constraint(x, pltpu.VMEM)


def on_device(train_points, targets, inverse_factor, counts, membership, test_points):
    cols = lax.axis_size("col")
    rows = lax.axis_size("row")
    slots = min(8, rows) // 2
    blocks_own, features, block = test_points.shape
    half = train_points.shape[2]
    points = 2 * half
    scale = math.log2(math.e) / features
    swap = [(i, i ^ 1) for i in range(cols)]
    step = 128
    in_hbm = pl.BlockSpec(memory_space=pltpu.HBM)
    in_vmem = pl.BlockSpec(memory_space=pltpu.VMEM)
    held = features + SUBLANES

    outgoing, packed, wanted = pl.pallas_call(
        send_kernel,
        out_shape=(pltpu.VMEM((rows, features, block), F32), pltpu.VMEM((held, half), F32), pltpu.VMEM((blocks_own, rows, LANES), F32)),
        in_specs=[in_hbm] * 4,
        out_specs=(in_vmem,) * 3,
        scratch_shapes=[pltpu.VMEM((rows, SUBLANES, membership.shape[2]), I32), pltpu.VMEM((blocks_own, features, block), F32), pltpu.SemaphoreType.DMA((4,))],
        compiler_params=pltpu.CompilerParams(vmem_limit_bytes=4 << 20),
        name="send",
    )(hbm(membership), hbm(test_points), hbm(train_points), hbm(targets))
    tests = lax.all_to_all(outgoing, "row", split_axis=0, concat_axis=0, tiled=True)
    other = lax.ppermute(packed, "col", swap)
    other_factor = lax.ppermute(inverse_factor[0], "col", swap)

    aug, y, table = pl.pallas_call(
        lambda *refs: points_kernel(*refs, features=features, factor=scale),
        out_shape=(
            pltpu.VMEM((points, 2 * LANES), BF16),
            pltpu.VMEM((2, points, LANES), BF16),
            pltpu.VMEM((slots, rows, LANES), F32),
        ),
        in_specs=[in_hbm] * 2 + [in_vmem] * 2,
        out_specs=(in_vmem,) * 3,
        scratch_shapes=[
            pltpu.VMEM((SUBLANES, membership.shape[2]), I32),
            pltpu.VMEM(counts.shape, I32),
            pltpu.VMEM((points, LANES), F32),
            pltpu.VMEM((points, LANES), F32),
            pltpu.VMEM((points, LANES), F32),
            pltpu.SemaphoreType.DMA((2,)),
        ],
        compiler_params=pltpu.CompilerParams(vmem_limit_bytes=16 << 20),
        name="points",
    )(hbm(membership), hbm(counts), vmem(packed), vmem(other))
    held_factor = (2 * step, first_column(half // step, step))
    fh, fl, alpha = pl.pallas_call(
        lambda *refs: factor_kernel(*refs, step=step),
        out_shape=(
            pltpu.VMEM(held_factor, BF16),
            pltpu.VMEM(held_factor, BF16),
            pltpu.VMEM((SUBLANES, points), F32),
        ),
        in_specs=[in_hbm] + [in_vmem] * 2,
        out_specs=(in_vmem,) * 3,
        scratch_shapes=[pltpu.VMEM((half, points), F32), pltpu.SemaphoreType.DMA((half // step,))],
        compiler_params=pltpu.CompilerParams(vmem_limit_bytes=16 << 20),
        name="factor",
    )(hbm(inverse_factor), vmem(other_factor), vmem(y))
    parts = pl.pallas_call(
        lambda *refs: expert_kernel(*refs, scale=scale, step=2 * step),
        out_shape=pltpu.VMEM((rows, 2, block), F32),
        in_specs=[in_vmem] * 6,
        out_specs=in_vmem,
        scratch_shapes=[pltpu.VMEM((points, slots * block), BF16)] * 2,
        compiler_params=pltpu.CompilerParams(vmem_limit_bytes=16 << 20),
        name="expert",
    )(vmem(aug), vmem(fh), vmem(fl), vmem(alpha), vmem(table), vmem(tests))
    arrived = lax.all_to_all(parts, "row", split_axis=0, concat_axis=0, tiled=True)
    spread = pl.pallas_call(
        owner_kernel,
        out_shape=pltpu.VMEM((cols, 2 * blocks_own, block), F32),
        in_specs=[in_vmem] * 2,
        out_specs=in_vmem,
        compiler_params=pltpu.CompilerParams(vmem_limit_bytes=4 << 20),
        name="owner",
    )(vmem(wanted), vmem(arrived))
    shares = lax.all_to_all(spread, "col", split_axis=0, concat_axis=0, tiled=True)
    return pl.pallas_call(
        final_kernel,
        out_shape=(jax.ShapeDtypeStruct((blocks_own, block), F32),) * 2,
        in_specs=[in_vmem],
        out_specs=(in_vmem,) * 2,
        compiler_params=pltpu.CompilerParams(vmem_limit_bytes=4 << 20),
        name="final",
    )(vmem(shares))


def solution(mesh):
    in_specs = (
        P("row", None, "col"),
        P("row", "col"),
        P("row", "col", None),
        P("row", None),
        P(),
        P("row", None, None),
    )
    out_specs = (P("row", None), P("row", None))

    return jax.shard_map(on_device, mesh=mesh, in_specs=in_specs, out_specs=out_specs, check_vma=False)
```

```python
import math

import jax
import jax.numpy as jnp
from jax import lax
from jax.experimental import pallas as pl
from jax.experimental.pallas import tpu as pltpu
from jax.sharding import PartitionSpec as P

SIGNAL = 1.0
NOISE = 0.1
BF16 = jnp.bfloat16
F32 = jnp.float32
I32 = jnp.int32
LANES = 128
SUBLANES = 8
GROUP = 4


def three_parts(v):
    high = v.astype(BF16).astype(F32)
    rest = v - high
    mid = rest.astype(BF16).astype(F32)
    return high, mid, (rest - mid).astype(BF16).astype(F32)


def two_parts(v):
    high = v.astype(BF16)
    return high, (v - high.astype(F32)).astype(BF16)


def place():
    col = lax.axis_index("col")
    return lax.axis_index("row"), col // 2, col % 2


def send_kernel(member_hbm, counts_hbm, tests_hbm, points_hbm, targets_hbm,
                out_hbm, packed_ref, wanted_ref, slots_ref, valid_ref,
                member_ref, counts_ref, tests_ref, out_ref, sems):
    own_row, expert, parity = place()
    peers = member_hbm.shape[0]
    features = points_hbm.shape[1]
    blocks_own, part, _ = tests_ref.shape
    near = pl.multiple_of(expert // SUBLANES * SUBLANES, SUBLANES)
    mine_at = pl.multiple_of(parity * part, part)
    copies = [
        pltpu.make_async_copy(member_hbm.at[:, pl.ds(near, SUBLANES), :], member_ref, sems.at[0]),
        pltpu.make_async_copy(tests_hbm.at[:, pl.ds(mine_at, part), :], tests_ref, sems.at[1]),
        pltpu.make_async_copy(counts_hbm, counts_ref, sems.at[2]),
        pltpu.make_async_copy(points_hbm.at[0], packed_ref.at[0:features], sems.at[3]),
        pltpu.make_async_copy(targets_hbm, packed_ref.at[features : features + 1], sems.at[4]),
    ]
    for c in copies:
        c.start()
    copies[0].wait()
    member = member_ref[...].astype(F32)
    sub = lax.broadcasted_iota(I32, member.shape, 1)
    mine = jnp.sum(jnp.where(sub == expert - near, member, 0.0), axis=1)
    row = lax.broadcasted_iota(I32, mine.shape, 0)
    lane = lax.broadcasted_iota(I32, mine.shape, 1)
    wide = [
        jnp.broadcast_to(
            jnp.sum(jnp.where(lane == own_row * blocks_own + b, mine, 0.0), axis=1, keepdims=True), (peers, LANES)
        )
        for b in range(blocks_own)
    ]
    for b in range(blocks_own):
        wanted_ref[b] = wide[b]
    copies[1].wait()
    blocks = [tests_ref[b] for b in range(blocks_own)]
    for r in range(peers):
        total = blocks[0] * wide[0][r : r + 1]
        for b in range(1, blocks_own):
            total = total + blocks[b] * wide[b][r : r + 1]
        out_ref[r] = total
        if r % GROUP == GROUP - 1:
            at = slice(r + 1 - GROUP, r + 1)
            copies.append(pltpu.make_async_copy(out_ref.at[at], out_hbm.at[at], sems.at[len(copies)]))
            copies[-1].start()
    own = jnp.sum(jnp.where(row == own_row, mine, 0.0), axis=0, keepdims=True)
    inside = (lane >= row * blocks_own) & (lane < row * blocks_own + blocks_own)
    held = jnp.sum(jnp.where(inside, own, 0.0), axis=1, keepdims=True)
    before = jnp.sum(jnp.where(lane < row * blocks_own, own, 0.0), axis=1, keepdims=True)
    for s in range(slots_ref.shape[0]):
        taken = (before == float(s)) & (held > 0.5)
        slots_ref[s] = jnp.broadcast_to(jnp.where(taken, 1.0, 0.0), (peers, LANES))
    copies[2].wait()
    counts = counts_ref[...]
    lane = lax.broadcasted_iota(I32, counts.shape, 1)
    valid = jnp.sum(jnp.where(lane == expert, counts, 0).astype(F32), axis=1, keepdims=True)
    valid_ref[...] = jnp.broadcast_to(valid, valid_ref.shape)
    for c in copies[3:]:
        c.wait()


def pick_kernel(slots_ref, tests_ref, mine_ref, theirs_ref):
    _, _, parity = place()
    peers, _, block = tests_ref.shape
    for m in range(slots_ref.shape[0] // 2):
        for odd, ref in ((parity, mine_ref), (1 - parity, theirs_ref)):
            s = slots_ref[2 * m + odd]
            total = tests_ref[0] * s[0:1]
            for r in range(1, peers):
                total = total + tests_ref[r] * s[r : r + 1]
            ref[:, m * block : m * block + block] = total


def first_column(a, step):
    return step * a * (a + 1)


def factor_copies(f_hbm, f_ref, sems, step):
    blocks = [(slice(step * a, step * a + step), slice(0, 2 * step * (a + 1))) for a in range(f_ref.shape[0] // step)]
    return [pltpu.make_async_copy(f_hbm.at[(0, *at)], f_ref.at[at], sems.at[a]) for a, at in enumerate(blocks)]


def factor_block(f_ref, a, step):
    return f_ref[step * a : step * a + step, 0 : 2 * step * (a + 1)]


def add_alpha(sums, f, parts, y_ref):
    rows, reach = f.shape
    w = jnp.dot(parts[0], y_ref[0:reach], preferred_element_type=F32)
    w = w + jnp.dot(parts[1], y_ref[0:reach], preferred_element_type=F32)
    w = w + pltpu.roll(w, LANES // 2, 1)
    for c in range(reach // LANES):
        part = f[:, c * LANES : c * LANES + LANES] * w
        sums[c] = sums[c] + jnp.sum(part.reshape(rows // SUBLANES, SUBLANES, LANES), axis=0)


def points_kernel(valid_ref, own_ref, other_ref, f_hbm, aug_ref, y_ref, alpha_ref,
                  first_ref, second_ref, third_ref, f_ref, sems, *, features, factor, step):
    _, _, parity = place()
    half = own_ref.shape[1]
    coming = factor_copies(f_hbm, f_ref, sems, step)
    for c in coming:
        c.start()
    valid = valid_ref[0:1, 0:1]

    def columns(ref, odd):
        points, y = ref[0:features, :], ref[features : features + 1, :]
        where = 2 * lax.broadcasted_iota(I32, (1, half), 1) + odd
        alive = where.astype(F32) < valid
        scaled = jnp.where(alive, points * (2.0 * factor), 0.0)
        square = jnp.where(alive, -factor * jnp.sum(points * points, axis=0, keepdims=True), -1e9)
        xh, xm, xl = three_parts(scaled)
        sh, sm, sl = three_parts(square)
        row = lax.broadcasted_iota(I32, (features, half), 0)
        last = jnp.where(row == 0, sh, jnp.where(row == 1, sm, jnp.where(row == 2, sl, 0.0)))
        last = jnp.where((row >= 3) & (row < 6), 1.0, last)
        wide = [xh, xh, xm, xm, xh, xl, last, jnp.zeros_like(xh), jnp.broadcast_to(y, (LANES, half))]
        return jnp.concatenate(wide, axis=0)

    own = columns(own_ref, parity)
    other = columns(other_ref, 1 - parity)
    first = jnp.where(parity == 0, own, other)
    second = jnp.where(parity == 0, other, own)
    for c, ref in enumerate((first_ref, second_ref, third_ref)):
        at = slice(c * LANES, c * LANES + LANES)
        ref[pl.ds(0, half, 2), :] = first[at].T
        ref[pl.ds(1, half, 2), :] = second[at].T
    aug_ref[:, 0:LANES] = first_ref[...].astype(BF16)
    aug_ref[:, LANES : 2 * LANES] = second_ref[...].astype(BF16)
    y = third_ref[...]
    yh = y.astype(BF16).astype(F32)
    lane = lax.broadcasted_iota(I32, y.shape, 1)
    y_ref[...] = jnp.where(lane < LANES // 2, yh, y - yh).astype(BF16)
    sums = [jnp.zeros((SUBLANES, LANES), F32) for _ in range(2 * half // LANES)]
    for a, c in enumerate(coming):
        c.wait()
        f = factor_block(f_ref, a, step)
        add_alpha(sums, f, two_parts(f), y_ref)
    for c, part in enumerate(sums):
        alpha_ref[:, c * LANES : c * LANES + LANES] = part


def factor_kernel(own_f_hbm, other_f_ref, y_ref, own_alpha_ref, fh_ref, fl_ref, alpha_ref, own_f_ref, sems, *, step):
    coming = factor_copies(own_f_hbm, own_f_ref, sems, step)
    for c in coming:
        c.start()
    sums = [own_alpha_ref[:, c : c + LANES] for c in range(0, y_ref.shape[0], LANES)]
    for which, f_ref in ((1, other_f_ref), (0, own_f_ref)):
        rows = slice(step * which, step * which + step)
        for a, c in enumerate(coming):
            if which == 0:
                c.wait()
            f = factor_block(f_ref, a, step)
            parts = two_parts(f)
            at = slice(first_column(a, step), first_column(a + 1, step))
            fh_ref[rows, at], fl_ref[rows, at] = parts
            if which == 1:
                add_alpha(sums, f, parts, y_ref)
    for c, part in enumerate(sums):
        alpha_ref[:, c * LANES : c * LANES + LANES] = jnp.broadcast_to(jnp.sum(part, axis=0, keepdims=True), (SUBLANES, LANES))


def expert_kernel(aug_ref, fh_ref, fl_ref, alpha_ref, slots_ref, mine_ref, theirs_ref, out_ref, kh_ref, kl_ref, *, scale, step):
    _, _, parity = place()
    points = aug_ref.shape[0]
    peers = slots_ref.shape[1]
    slots = slots_ref.shape[0] // 2
    part, width = mine_ref.shape
    features, block = 2 * part, width // slots
    mine, theirs = mine_ref[...], theirs_ref[...]
    t = jnp.concatenate([jnp.where(parity == 0, mine, theirs), jnp.where(parity == 0, theirs, mine)], axis=0)
    th, tm, tl = three_parts(t)
    square = -scale * jnp.sum(t * t, axis=0, keepdims=True)
    sh, sm, sl = three_parts(square)
    row = lax.broadcasted_iota(I32, (features, width), 0)
    last = jnp.where(row == 3, sh, jnp.where(row == 4, sm, jnp.where(row == 5, sl, 0.0)))
    last = jnp.where(row < 3, 1.0, last)
    taug = jnp.concatenate([th, tm, th, tm, tl, th, last, jnp.zeros_like(th)], axis=0).astype(BF16)
    quad = jnp.zeros((1, width), F32)
    mean = jnp.zeros((1, width), F32)
    for a in range(points // step):
        at = slice(a * step, a * step + step)
        k = jnp.exp2(jnp.dot(aug_ref[at, :], taug, preferred_element_type=F32))
        kh, kl = two_parts(k)
        kh_ref[at, :] = kh
        kl_ref[at, :] = kl
        alpha = jnp.concatenate(
            [
                jnp.broadcast_to(alpha_ref[0:1, c : c + LANES], (LANES, LANES)).T
                for c in range(a * step, a * step + step, LANES)
            ],
            axis=0,
        )
        mean = mean + jnp.sum(k * jnp.concatenate([alpha] * slots, axis=1), axis=0, keepdims=True)
    for a in range(points // step):
        reach = step * (a + 1)
        at = slice(first_column(a, step // 2), first_column(a, step // 2) + reach)
        solved = jnp.dot(fh_ref[:, at], kh_ref[0:reach, :], preferred_element_type=F32)
        solved = solved + jnp.dot(fl_ref[:, at], kh_ref[0:reach, :], preferred_element_type=F32)
        solved = solved + jnp.dot(fh_ref[:, at], kl_ref[0:reach, :], preferred_element_type=F32)
        quad = quad + jnp.sum(solved * solved, axis=0, keepdims=True)
    variance = NOISE + jnp.maximum(SIGNAL - quad, 0.0)
    gap = 0.5 * (math.log(SIGNAL + NOISE) - jnp.log(variance))
    weight = gap / variance
    both = jnp.concatenate([weight * mean, weight], axis=0)
    for r in range(peers):
        total = both[:, 0:block] * slots_ref[parity, r : r + 1]
        for m in range(1, slots):
            total = total + both[:, m * block : m * block + block] * slots_ref[2 * m + parity, r : r + 1]
        out_ref[r] = total


def owner_kernel(wanted_ref, parts_ref, out_ref):
    peers, _, _ = parts_ref.shape
    blocks = wanted_ref.shape[0]
    num, wgt = [], []
    for b in range(blocks):
        total = parts_ref[0] * wanted_ref[b, 0:1]
        for r in range(1, peers):
            total = total + parts_ref[r] * wanted_ref[b, r : r + 1]
        num.append(total[0:1])
        wgt.append(total[1:2])
    tile = jnp.concatenate(num + wgt, axis=0)
    for j in range(out_ref.shape[0]):
        out_ref[j] = tile


def final_kernel(parts_ref, mean_ref, var_ref):
    parts = [parts_ref[j] for j in range(parts_ref.shape[0])]
    while len(parts) > 1:
        parts = [parts[i] + parts[i + 1] for i in range(0, len(parts), 2)]
    total = parts[0]
    blocks = mean_ref.shape[0]
    precision = 1.0 / (SIGNAL + NOISE) + total[blocks:]
    mean_ref[...] = total[0:blocks] / precision
    var_ref[...] = 1.0 / precision


def hbm(x):
    return pltpu.with_memory_space_constraint(x, pltpu.HBM)


def vmem(x):
    return pltpu.with_memory_space_constraint(x, pltpu.VMEM)


def on_device(train_points, targets, inverse_factor, counts, membership, test_points):
    cols = lax.axis_size("col")
    rows = lax.axis_size("row")
    slots = min(8, rows) // 2
    blocks_own, features, block = test_points.shape
    half = train_points.shape[2]
    points = 2 * half
    scale = math.log2(math.e) / features
    swap = [(i, i ^ 1) for i in range(cols)]
    step = 128
    in_hbm = pl.BlockSpec(memory_space=pltpu.HBM)
    in_vmem = pl.BlockSpec(memory_space=pltpu.VMEM)
    held = features + SUBLANES

    outgoing, packed, wanted, table, valid = pl.pallas_call(
        send_kernel,
        out_shape=(
            pltpu.HBM((rows, features // 2, block), F32),
            pltpu.VMEM((held, half), F32),
            pltpu.VMEM((blocks_own, rows, LANES), F32),
            pltpu.VMEM((2 * slots, rows, LANES), F32),
            pltpu.VMEM((SUBLANES, LANES), F32),
        ),
        in_specs=[in_hbm] * 5,
        out_specs=(in_hbm,) + (in_vmem,) * 4,
        scratch_shapes=[
            pltpu.VMEM((rows, SUBLANES, membership.shape[2]), I32),
            pltpu.VMEM(counts.shape, I32),
            pltpu.VMEM((blocks_own, features // 2, block), F32),
            pltpu.VMEM((rows, features // 2, block), F32),
            pltpu.SemaphoreType.DMA((5 + rows // GROUP,)),
        ],
        compiler_params=pltpu.CompilerParams(vmem_limit_bytes=4 << 20),
        name="send",
    )(hbm(membership), hbm(counts), hbm(test_points), hbm(train_points), hbm(targets))
    tests = lax.all_to_all(outgoing, "row", split_axis=0, concat_axis=0, tiled=True)
    other = lax.ppermute(packed, "col", swap)
    other_factor = lax.ppermute(inverse_factor[0], "col", swap)

    chunks = half // step
    reach = first_column(chunks, step)
    held_f = [pltpu.VMEM((half, points), F32), pltpu.SemaphoreType.DMA((chunks,))]
    aug, y, own_alpha = pl.pallas_call(
        lambda *refs: points_kernel(*refs, features=features, factor=scale, step=step),
        out_shape=(
            pltpu.VMEM((points, 2 * LANES), BF16),
            pltpu.VMEM((points, LANES), BF16),
            pltpu.VMEM((SUBLANES, points), F32),
        ),
        in_specs=[in_vmem] * 3 + [in_hbm],
        out_specs=(in_vmem,) * 3,
        scratch_shapes=[pltpu.VMEM((points, LANES), F32)] * 3 + held_f,
        compiler_params=pltpu.CompilerParams(vmem_limit_bytes=16 << 20),
        name="points",
    )(vmem(valid), vmem(packed), vmem(other), hbm(inverse_factor))
    tests, aug = lax.optimization_barrier((tests, aug))
    mine, theirs = pl.pallas_call(
        pick_kernel,
        out_shape=(pltpu.VMEM((features // 2, slots * block), F32),) * 2,
        in_specs=[in_vmem] * 2,
        out_specs=(in_vmem,) * 2,
        compiler_params=pltpu.CompilerParams(vmem_limit_bytes=4 << 20),
        name="pick",
    )(vmem(table), vmem(tests))
    theirs = lax.ppermute(theirs, "col", swap)
    fh, fl, alpha = pl.pallas_call(
        lambda *refs: factor_kernel(*refs, step=step),
        out_shape=(
            pltpu.VMEM((2 * step, reach), BF16),
            pltpu.VMEM((2 * step, reach), BF16),
            pltpu.VMEM((SUBLANES, points), F32),
        ),
        in_specs=[in_hbm] + [in_vmem] * 3,
        out_specs=(in_vmem,) * 3,
        scratch_shapes=held_f,
        compiler_params=pltpu.CompilerParams(vmem_limit_bytes=12 << 20),
        name="factor",
    )(hbm(inverse_factor), vmem(other_factor), vmem(y), vmem(own_alpha))
    parts = pl.pallas_call(
        lambda *refs: expert_kernel(*refs, scale=scale, step=2 * step),
        out_shape=pltpu.VMEM((rows, 2, block), F32),
        in_specs=[in_vmem] * 7,
        out_specs=in_vmem,
        scratch_shapes=[pltpu.VMEM((points, slots * block), BF16)] * 2,
        compiler_params=pltpu.CompilerParams(vmem_limit_bytes=16 << 20),
        name="expert",
    )(*map(vmem, (aug, fh, fl, alpha, table, mine, theirs)))
    arrived = lax.all_to_all(parts, "row", split_axis=0, concat_axis=0, tiled=True)
    spread = pl.pallas_call(
        owner_kernel,
        out_shape=pltpu.VMEM((cols, 2 * blocks_own, block), F32),
        in_specs=[in_vmem] * 2,
        out_specs=in_vmem,
        compiler_params=pltpu.CompilerParams(vmem_limit_bytes=4 << 20),
        name="owner",
    )(vmem(wanted), vmem(arrived))
    shares = lax.all_to_all(spread, "col", split_axis=0, concat_axis=0, tiled=True)
    return pl.pallas_call(
        final_kernel,
        out_shape=(jax.ShapeDtypeStruct((blocks_own, block), F32),) * 2,
        in_specs=[in_vmem],
        out_specs=(in_vmem,) * 2,
        compiler_params=pltpu.CompilerParams(vmem_limit_bytes=4 << 20),
        name="final",
    )(vmem(shares))


def solution(mesh):
    in_specs = (
        P("row", None, "col"),
        P("row", "col"),
        P("row", "col", None),
        P("row", None),
        P(),
        P("row", None, None),
    )
    out_specs = (P("row", None), P("row", None))

    return jax.shard_map(on_device, mesh=mesh, in_specs=in_specs, out_specs=out_specs, check_vma=False)
```

```python
import math

import jax
import jax.numpy as jnp
from jax import lax
from jax.experimental import pallas as pl
from jax.experimental.pallas import tpu as pltpu
from jax.sharding import PartitionSpec as P

SIGNAL = 1.0
NOISE = 0.1
BF16 = jnp.bfloat16
F32 = jnp.float32
I32 = jnp.int32
LANES = 128
SUBLANES = 8
GROUP = 4


def three_parts(v):
    high = v.astype(BF16).astype(F32)
    rest = v - high
    mid = rest.astype(BF16).astype(F32)
    return high, mid, (rest - mid).astype(BF16).astype(F32)


def two_parts(v):
    high = v.astype(BF16)
    return high, (v - high.astype(F32)).astype(BF16)


def place():
    col = lax.axis_index("col")
    return lax.axis_index("row"), col // 2, col % 2


def send_kernel(member_hbm, counts_hbm, tests_hbm, points_hbm, targets_hbm,
                out_hbm, packed_ref, wanted_ref, slots_ref, valid_ref,
                member_ref, counts_ref, tests_ref, out_ref, sems):
    own_row, expert, parity = place()
    peers = member_hbm.shape[0]
    features = points_hbm.shape[1]
    blocks_own, part, _ = tests_ref.shape
    mine_at = pl.multiple_of(parity * part, part)
    copies = [
        pltpu.make_async_copy(member_hbm.at[:, pl.ds(expert, 1), :], member_ref, sems.at[0]),
        pltpu.make_async_copy(tests_hbm.at[:, pl.ds(mine_at, part), :], tests_ref, sems.at[1]),
        pltpu.make_async_copy(counts_hbm, counts_ref, sems.at[2]),
        pltpu.make_async_copy(points_hbm.at[0], packed_ref.at[0:features], sems.at[3]),
        pltpu.make_async_copy(targets_hbm, packed_ref.at[features : features + 1], sems.at[4]),
    ]
    for c in copies:
        c.start()
    copies[0].wait()
    mine = jnp.sum(member_ref[...].astype(F32), axis=1)
    row = lax.broadcasted_iota(I32, mine.shape, 0)
    lane = lax.broadcasted_iota(I32, mine.shape, 1)
    wide = [
        jnp.broadcast_to(
            jnp.sum(jnp.where(lane == own_row * blocks_own + b, mine, 0.0), axis=1, keepdims=True), (peers, LANES)
        )
        for b in range(blocks_own)
    ]
    for b in range(blocks_own):
        wanted_ref[b] = wide[b]
    copies[1].wait()
    blocks = [tests_ref[b] for b in range(blocks_own)]
    for r in range(peers):
        total = blocks[0] * wide[0][r : r + 1]
        for b in range(1, blocks_own):
            total = total + blocks[b] * wide[b][r : r + 1]
        out_ref[r] = total
        if r % GROUP == GROUP - 1:
            at = slice(r + 1 - GROUP, r + 1)
            copies.append(pltpu.make_async_copy(out_ref.at[at], out_hbm.at[at], sems.at[len(copies)]))
            copies[-1].start()
    own = jnp.sum(jnp.where(row == own_row, mine, 0.0), axis=0, keepdims=True)
    inside = (lane >= row * blocks_own) & (lane < row * blocks_own + blocks_own)
    held = jnp.sum(jnp.where(inside, own, 0.0), axis=1, keepdims=True)
    before = jnp.sum(jnp.where(lane < row * blocks_own, own, 0.0), axis=1, keepdims=True)
    for s in range(slots_ref.shape[0]):
        taken = (before == float(s)) & (held > 0.5)
        slots_ref[s] = jnp.broadcast_to(jnp.where(taken, 1.0, 0.0), (peers, LANES))
    copies[2].wait()
    counts = counts_ref[...]
    lane = lax.broadcasted_iota(I32, counts.shape, 1)
    valid = jnp.sum(jnp.where(lane == expert, counts, 0).astype(F32), axis=1, keepdims=True)
    valid_ref[...] = jnp.broadcast_to(valid, valid_ref.shape)
    for c in copies[3:]:
        c.wait()


def pick_kernel(slots_ref, tests_ref, mine_ref, theirs_ref):
    _, _, parity = place()
    peers, _, block = tests_ref.shape
    for m in range(slots_ref.shape[0] // 2):
        for odd, ref in ((parity, mine_ref), (1 - parity, theirs_ref)):
            s = slots_ref[2 * m + odd]
            total = tests_ref[0] * s[0:1]
            for r in range(1, peers):
                total = total + tests_ref[r] * s[r : r + 1]
            ref[:, m * block : m * block + block] = total


def first_column(a, step):
    return step * a * (a + 1)


def factor_copies(f_hbm, f_ref, sems, step):
    blocks = [(slice(step * a, step * a + step), slice(0, 2 * step * (a + 1))) for a in range(f_ref.shape[0] // step)]
    return [pltpu.make_async_copy(f_hbm.at[(0, *at)], f_ref.at[at], sems.at[a]) for a, at in enumerate(blocks)]


def factor_block(f_ref, a, step):
    return f_ref[step * a : step * a + step, 0 : 2 * step * (a + 1)]


def add_alpha(sums, f, parts, y_ref):
    rows, reach = f.shape
    w = jnp.dot(parts[0], y_ref[0:reach], preferred_element_type=F32)
    w = w + jnp.dot(parts[1], y_ref[0:reach], preferred_element_type=F32)
    w = w + pltpu.roll(w, LANES // 2, 1)
    for c in range(reach // LANES):
        part = f[:, c * LANES : c * LANES + LANES] * w
        sums[c] = sums[c] + jnp.sum(part.reshape(rows // SUBLANES, SUBLANES, LANES), axis=0)


def points_kernel(valid_ref, own_ref, other_ref, f_hbm, aug_ref, y_ref, alpha_ref,
                  first_ref, second_ref, third_ref, f_ref, sems, *, features, factor, step):
    _, _, parity = place()
    half = own_ref.shape[1]
    coming = factor_copies(f_hbm, f_ref, sems, step)
    for c in coming:
        c.start()
    valid = valid_ref[0:1, 0:1]

    def columns(ref, odd):
        points, y = ref[0:features, :], ref[features : features + 1, :]
        where = 2 * lax.broadcasted_iota(I32, (1, half), 1) + odd
        alive = where.astype(F32) < valid
        scaled = jnp.where(alive, points * (2.0 * factor), 0.0)
        square = jnp.where(alive, -factor * jnp.sum(points * points, axis=0, keepdims=True), -1e9)
        xh, xm, xl = three_parts(scaled)
        sh, sm, sl = three_parts(square)
        row = lax.broadcasted_iota(I32, (features, half), 0)
        last = jnp.where(row == 0, sh, jnp.where(row == 1, sm, jnp.where(row == 2, sl, 0.0)))
        last = jnp.where((row >= 3) & (row < 6), 1.0, last)
        wide = [xh, xh, xm, xm, xh, xl, last, jnp.zeros_like(xh), jnp.broadcast_to(y, (LANES, half))]
        return jnp.concatenate(wide, axis=0)

    own = columns(own_ref, parity)
    other = columns(other_ref, 1 - parity)
    first = jnp.where(parity == 0, own, other)
    second = jnp.where(parity == 0, other, own)
    for c, ref in enumerate((first_ref, second_ref, third_ref)):
        at = slice(c * LANES, c * LANES + LANES)
        ref[pl.ds(0, half, 2), :] = first[at].T
        ref[pl.ds(1, half, 2), :] = second[at].T
    aug_ref[:, 0:LANES] = first_ref[...].astype(BF16)
    aug_ref[:, LANES : 2 * LANES] = second_ref[...].astype(BF16)
    y = third_ref[...]
    yh = y.astype(BF16).astype(F32)
    lane = lax.broadcasted_iota(I32, y.shape, 1)
    y_ref[...] = jnp.where(lane < LANES // 2, yh, y - yh).astype(BF16)
    sums = [jnp.zeros((SUBLANES, LANES), F32) for _ in range(2 * half // LANES)]
    for a, c in enumerate(coming):
        c.wait()
        f = factor_block(f_ref, a, step)
        add_alpha(sums, f, two_parts(f), y_ref)
    for c, part in enumerate(sums):
        alpha_ref[:, c * LANES : c * LANES + LANES] = part


def factor_kernel(own_f_hbm, other_f_ref, y_ref, own_alpha_ref, fh_ref, fl_ref, alpha_ref, own_f_ref, sems, *, step):
    coming = factor_copies(own_f_hbm, own_f_ref, sems, step)
    for c in coming:
        c.start()
    sums = [own_alpha_ref[:, c : c + LANES] for c in range(0, y_ref.shape[0], LANES)]
    for which, f_ref in ((1, other_f_ref), (0, own_f_ref)):
        rows = slice(step * which, step * which + step)
        for a, c in enumerate(coming):
            if which == 0:
                c.wait()
            f = factor_block(f_ref, a, step)
            parts = two_parts(f)
            at = slice(first_column(a, step), first_column(a + 1, step))
            fh_ref[rows, at], fl_ref[rows, at] = parts
            if which == 1:
                add_alpha(sums, f, parts, y_ref)
    for c, part in enumerate(sums):
        alpha_ref[:, c * LANES : c * LANES + LANES] = jnp.broadcast_to(jnp.sum(part, axis=0, keepdims=True), (SUBLANES, LANES))


def expert_kernel(aug_ref, fh_ref, fl_ref, alpha_ref, slots_ref, mine_ref, theirs_ref, out_ref, kh_ref, kl_ref, *, scale, step):
    _, _, parity = place()
    points = aug_ref.shape[0]
    peers = slots_ref.shape[1]
    slots = slots_ref.shape[0] // 2
    part, width = mine_ref.shape
    features, block = 2 * part, width // slots
    mine, theirs = mine_ref[...], theirs_ref[...]
    t = jnp.concatenate([jnp.where(parity == 0, mine, theirs), jnp.where(parity == 0, theirs, mine)], axis=0)
    th, tm, tl = three_parts(t)
    square = -scale * jnp.sum(t * t, axis=0, keepdims=True)
    sh, sm, sl = three_parts(square)
    row = lax.broadcasted_iota(I32, (features, width), 0)
    last = jnp.where(row == 3, sh, jnp.where(row == 4, sm, jnp.where(row == 5, sl, 0.0)))
    last = jnp.where(row < 3, 1.0, last)
    taug = jnp.concatenate([th, tm, th, tm, tl, th, last, jnp.zeros_like(th)], axis=0).astype(BF16)
    quad = jnp.zeros((1, width), F32)
    mean = jnp.zeros((1, width), F32)
    for a in range(points // step):
        at = slice(a * step, a * step + step)
        k = jnp.exp2(jnp.dot(aug_ref[at, :], taug, preferred_element_type=F32))
        kh, kl = two_parts(k)
        kh_ref[at, :] = kh
        kl_ref[at, :] = kl
        alpha = jnp.concatenate(
            [
                jnp.broadcast_to(alpha_ref[0:1, c : c + LANES], (LANES, LANES)).T
                for c in range(a * step, a * step + step, LANES)
            ],
            axis=0,
        )
        mean = mean + jnp.sum(k * jnp.concatenate([alpha] * slots, axis=1), axis=0, keepdims=True)
    for a in range(points // step):
        reach = step * (a + 1)
        at = slice(first_column(a, step // 2), first_column(a, step // 2) + reach)
        solved = jnp.dot(fh_ref[:, at], kh_ref[0:reach, :], preferred_element_type=F32)
        solved = solved + jnp.dot(fl_ref[:, at], kh_ref[0:reach, :], preferred_element_type=F32)
        solved = solved + jnp.dot(fh_ref[:, at], kl_ref[0:reach, :], preferred_element_type=F32)
        quad = quad + jnp.sum(solved * solved, axis=0, keepdims=True)
    variance = NOISE + jnp.maximum(SIGNAL - quad, 0.0)
    gap = 0.5 * (math.log(SIGNAL + NOISE) - jnp.log(variance))
    weight = gap / variance
    both = jnp.concatenate([weight * mean, weight], axis=0)
    for r in range(peers):
        total = both[:, 0:block] * slots_ref[parity, r : r + 1]
        for m in range(1, slots):
            total = total + both[:, m * block : m * block + block] * slots_ref[2 * m + parity, r : r + 1]
        out_ref[r] = total


def owner_kernel(wanted_ref, parts_ref, out_ref):
    peers, _, _ = parts_ref.shape
    blocks = wanted_ref.shape[0]
    num, wgt = [], []
    for b in range(blocks):
        total = parts_ref[0] * wanted_ref[b, 0:1]
        for r in range(1, peers):
            total = total + parts_ref[r] * wanted_ref[b, r : r + 1]
        num.append(total[0:1])
        wgt.append(total[1:2])
    tile = jnp.concatenate(num + wgt, axis=0)
    for j in range(out_ref.shape[0]):
        out_ref[j] = tile


def final_kernel(parts_ref, mean_ref, var_ref):
    parts = [parts_ref[j] for j in range(parts_ref.shape[0])]
    while len(parts) > 1:
        parts = [parts[i] + parts[i + 1] for i in range(0, len(parts), 2)]
    total = parts[0]
    blocks = mean_ref.shape[0]
    precision = 1.0 / (SIGNAL + NOISE) + total[blocks:]
    mean_ref[...] = total[0:blocks] / precision
    var_ref[...] = 1.0 / precision


def hbm(x):
    return pltpu.with_memory_space_constraint(x, pltpu.HBM)


def vmem(x):
    return pltpu.with_memory_space_constraint(x, pltpu.VMEM)


def on_device(train_points, targets, inverse_factor, counts, membership, test_points):
    cols = lax.axis_size("col")
    rows = lax.axis_size("row")
    slots = min(8, rows) // 2
    blocks_own, features, block = test_points.shape
    half = train_points.shape[2]
    points = 2 * half
    scale = math.log2(math.e) / features
    swap = [(i, i ^ 1) for i in range(cols)]
    step = 128
    in_hbm = pl.BlockSpec(memory_space=pltpu.HBM)
    in_vmem = pl.BlockSpec(memory_space=pltpu.VMEM)
    held = features + SUBLANES

    outgoing, packed, wanted, table, valid = pl.pallas_call(
        send_kernel,
        out_shape=(
            pltpu.HBM((rows, features // 2, block), F32),
            pltpu.VMEM((held, half), F32),
            pltpu.VMEM((blocks_own, rows, LANES), F32),
            pltpu.VMEM((2 * slots, rows, LANES), F32),
            pltpu.VMEM((SUBLANES, LANES), F32),
        ),
        in_specs=[in_hbm] * 5,
        out_specs=(in_hbm,) + (in_vmem,) * 4,
        scratch_shapes=[
            pltpu.VMEM((rows, 1, membership.shape[2]), I32),
            pltpu.VMEM(counts.shape, I32),
            pltpu.VMEM((blocks_own, features // 2, block), F32),
            pltpu.VMEM((rows, features // 2, block), F32),
            pltpu.SemaphoreType.DMA((5 + rows // GROUP,)),
        ],
        compiler_params=pltpu.CompilerParams(vmem_limit_bytes=4 << 20),
        name="send",
    )(hbm(membership), hbm(counts), hbm(test_points), hbm(train_points), hbm(targets))
    tests = lax.all_to_all(outgoing, "row", split_axis=0, concat_axis=0, tiled=True)
    other = lax.ppermute(packed, "col", swap)
    other_factor = lax.ppermute(inverse_factor[0], "col", swap)

    chunks = half // step
    reach = first_column(chunks, step)
    held_f = [pltpu.VMEM((half, points), F32), pltpu.SemaphoreType.DMA((chunks,))]
    aug, y, own_alpha = pl.pallas_call(
        lambda *refs: points_kernel(*refs, features=features, factor=scale, step=step),
        out_shape=(
            pltpu.VMEM((points, 2 * LANES), BF16),
            pltpu.VMEM((points, LANES), BF16),
            pltpu.VMEM((SUBLANES, points), F32),
        ),
        in_specs=[in_vmem] * 3 + [in_hbm],
        out_specs=(in_vmem,) * 3,
        scratch_shapes=[pltpu.VMEM((points, LANES), F32)] * 3 + held_f,
        compiler_params=pltpu.CompilerParams(vmem_limit_bytes=16 << 20),
        name="points",
    )(vmem(valid), vmem(packed), vmem(other), hbm(inverse_factor))
    tests, aug = lax.optimization_barrier((tests, aug))
    mine, theirs = pl.pallas_call(
        pick_kernel,
        out_shape=(pltpu.VMEM((features // 2, slots * block), F32),) * 2,
        in_specs=[in_vmem] * 2,
        out_specs=(in_vmem,) * 2,
        compiler_params=pltpu.CompilerParams(vmem_limit_bytes=4 << 20),
        name="pick",
    )(vmem(table), vmem(tests))
    theirs = lax.ppermute(theirs, "col", swap)
    fh, fl, alpha = pl.pallas_call(
        lambda *refs: factor_kernel(*refs, step=step),
        out_shape=(
            pltpu.VMEM((2 * step, reach), BF16),
            pltpu.VMEM((2 * step, reach), BF16),
            pltpu.VMEM((SUBLANES, points), F32),
        ),
        in_specs=[in_hbm] + [in_vmem] * 3,
        out_specs=(in_vmem,) * 3,
        scratch_shapes=held_f,
        compiler_params=pltpu.CompilerParams(vmem_limit_bytes=12 << 20),
        name="factor",
    )(hbm(inverse_factor), vmem(other_factor), vmem(y), vmem(own_alpha))
    parts = pl.pallas_call(
        lambda *refs: expert_kernel(*refs, scale=scale, step=2 * step),
        out_shape=pltpu.VMEM((rows, 2, block), F32),
        in_specs=[in_vmem] * 7,
        out_specs=in_vmem,
        scratch_shapes=[pltpu.VMEM((points, slots * block), BF16)] * 2,
        compiler_params=pltpu.CompilerParams(vmem_limit_bytes=16 << 20),
        name="expert",
    )(*map(vmem, (aug, fh, fl, alpha, table, mine, theirs)))
    arrived = lax.all_to_all(parts, "row", split_axis=0, concat_axis=0, tiled=True)
    spread = pl.pallas_call(
        owner_kernel,
        out_shape=pltpu.VMEM((cols, 2 * blocks_own, block), F32),
        in_specs=[in_vmem] * 2,
        out_specs=in_vmem,
        compiler_params=pltpu.CompilerParams(vmem_limit_bytes=4 << 20),
        name="owner",
    )(vmem(wanted), vmem(arrived))
    shares = lax.all_to_all(spread, "col", split_axis=0, concat_axis=0, tiled=True)
    return pl.pallas_call(
        final_kernel,
        out_shape=(jax.ShapeDtypeStruct((blocks_own, block), F32),) * 2,
        in_specs=[in_vmem],
        out_specs=(in_vmem,) * 2,
        compiler_params=pltpu.CompilerParams(vmem_limit_bytes=4 << 20),
        name="final",
    )(vmem(shares))


def solution(mesh):
    in_specs = (
        P("row", None, "col"),
        P("row", "col"),
        P("row", "col", None),
        P("row", None),
        P(),
        P("row", None, None),
    )
    out_specs = (P("row", None), P("row", None))

    return jax.shard_map(on_device, mesh=mesh, in_specs=in_specs, out_specs=out_specs, check_vma=False)
```

```python
import math

import jax
import jax.numpy as jnp
from jax import lax
from jax.experimental import pallas as pl
from jax.experimental.pallas import tpu as pltpu
from jax.sharding import PartitionSpec as P

SIGNAL = 1.0
NOISE = 0.1
BF16 = jnp.bfloat16
F32 = jnp.float32
I32 = jnp.int32
LANES = 128
SUBLANES = 8
GROUP = 4


def three_parts(v):
    high = v.astype(BF16).astype(F32)
    rest = v - high
    mid = rest.astype(BF16).astype(F32)
    return high, mid, (rest - mid).astype(BF16).astype(F32)


def two_parts(v):
    high = v.astype(BF16)
    return high, (v - high.astype(F32)).astype(BF16)


def place():
    col = lax.axis_index("col")
    return lax.axis_index("row"), col // 2, col % 2


def send_kernel(member_hbm, counts_hbm, tests_hbm, points_hbm, targets_hbm,
                out_hbm, packed_ref, wanted_ref, slots_ref, valid_ref,
                member_ref, counts_ref, tests_ref, out_ref, sems):
    own_row, expert, parity = place()
    peers = member_hbm.shape[0]
    features = points_hbm.shape[1]
    blocks_own, part, _ = tests_ref.shape
    near = pl.multiple_of(expert // SUBLANES * SUBLANES, SUBLANES)
    mine_at = pl.multiple_of(parity * part, part)
    copies = [
        pltpu.make_async_copy(member_hbm.at[:, pl.ds(near, SUBLANES), :], member_ref, sems.at[0]),
        pltpu.make_async_copy(tests_hbm.at[:, pl.ds(mine_at, part), :], tests_ref, sems.at[1]),
        pltpu.make_async_copy(counts_hbm, counts_ref, sems.at[2]),
        pltpu.make_async_copy(points_hbm.at[0], packed_ref.at[0:features], sems.at[3]),
        pltpu.make_async_copy(targets_hbm, packed_ref.at[features : features + 1], sems.at[4]),
    ]
    for c in copies:
        c.start()
    copies[0].wait()
    member = member_ref[...].astype(F32)
    sub = lax.broadcasted_iota(I32, member.shape, 1)
    mine = jnp.sum(jnp.where(sub == expert - near, member, 0.0), axis=1)
    row = lax.broadcasted_iota(I32, mine.shape, 0)
    lane = lax.broadcasted_iota(I32, mine.shape, 1)
    wide = [
        jnp.broadcast_to(
            jnp.sum(jnp.where(lane == own_row * blocks_own + b, mine, 0.0), axis=1, keepdims=True), (peers, LANES)
        )
        for b in range(blocks_own)
    ]
    for b in range(blocks_own):
        wanted_ref[b] = wide[b]
    copies[1].wait()
    blocks = [tests_ref[b] for b in range(blocks_own)]
    for r in range(peers):
        total = blocks[0] * wide[0][r : r + 1]
        for b in range(1, blocks_own):
            total = total + blocks[b] * wide[b][r : r + 1]
        out_ref[r] = total
        if r % GROUP == GROUP - 1:
            at = slice(r + 1 - GROUP, r + 1)
            copies.append(pltpu.make_async_copy(out_ref.at[at], out_hbm.at[at], sems.at[len(copies)]))
            copies[-1].start()
    own = jnp.sum(jnp.where(row == own_row, mine, 0.0), axis=0, keepdims=True)
    inside = (lane >= row * blocks_own) & (lane < row * blocks_own + blocks_own)
    held = jnp.sum(jnp.where(inside, own, 0.0), axis=1, keepdims=True)
    before = jnp.sum(jnp.where(lane < row * blocks_own, own, 0.0), axis=1, keepdims=True)
    for s in range(slots_ref.shape[0]):
        taken = (before == float(s)) & (held > 0.5)
        slots_ref[s] = jnp.broadcast_to(jnp.where(taken, 1.0, 0.0), (peers, LANES))
    copies[2].wait()
    counts = counts_ref[...]
    lane = lax.broadcasted_iota(I32, counts.shape, 1)
    valid = jnp.sum(jnp.where(lane == expert, counts, 0).astype(F32), axis=1, keepdims=True)
    valid_ref[...] = jnp.broadcast_to(valid, valid_ref.shape)
    for c in copies[3:]:
        c.wait()


def pick_kernel(slots_ref, tests_ref, mine_ref, theirs_ref):
    _, _, parity = place()
    peers, _, block = tests_ref.shape
    for m in range(slots_ref.shape[0] // 2):
        for odd, ref in ((parity, mine_ref), (1 - parity, theirs_ref)):
            s = slots_ref[2 * m + odd]
            total = tests_ref[0] * s[0:1]
            for r in range(1, peers):
                total = total + tests_ref[r] * s[r : r + 1]
            ref[:, m * block : m * block + block] = total


def first_column(a, step):
    return step * a * (a + 1)


def factor_copies(f_hbm, f_ref, sems, step):
    blocks = [(slice(step * a, step * a + step), slice(0, 2 * step * (a + 1))) for a in range(f_ref.shape[0] // step)]
    return [pltpu.make_async_copy(f_hbm.at[(0, *at)], f_ref.at[at], sems.at[a]) for a, at in enumerate(blocks)]


def factor_block(f_ref, a, step):
    return f_ref[step * a : step * a + step, 0 : 2 * step * (a + 1)]


def add_alpha(sums, f, parts, y_ref):
    rows, reach = f.shape
    w = jnp.dot(parts[0], y_ref[0:reach], preferred_element_type=F32)
    w = w + jnp.dot(parts[1], y_ref[0:reach], preferred_element_type=F32)
    w = w + pltpu.roll(w, LANES // 2, 1)
    for c in range(reach // LANES):
        part = f[:, c * LANES : c * LANES + LANES] * w
        sums[c] = sums[c] + jnp.sum(part.reshape(rows // SUBLANES, SUBLANES, LANES), axis=0)


def points_kernel(valid_ref, own_ref, other_ref, f_hbm, aug_ref, y_ref, alpha_ref,
                  first_ref, second_ref, third_ref, f_ref, sems, *, features, factor, step):
    _, _, parity = place()
    half = own_ref.shape[1]
    coming = factor_copies(f_hbm, f_ref, sems, step)
    for c in coming[::-1]:
        c.start()
    valid = valid_ref[0:1, 0:1]

    def columns(ref, odd):
        points, y = ref[0:features, :], ref[features : features + 1, :]
        where = 2 * lax.broadcasted_iota(I32, (1, half), 1) + odd
        alive = where.astype(F32) < valid
        scaled = jnp.where(alive, points * (2.0 * factor), 0.0)
        square = jnp.where(alive, -factor * jnp.sum(points * points, axis=0, keepdims=True), -1e9)
        xh, xm, xl = three_parts(scaled)
        sh, sm, sl = three_parts(square)
        row = lax.broadcasted_iota(I32, (features, half), 0)
        last = jnp.where(row == 0, sh, jnp.where(row == 1, sm, jnp.where(row == 2, sl, 0.0)))
        last = jnp.where((row >= 3) & (row < 6), 1.0, last)
        wide = [xh, xh, xm, xm, xh, xl, last, jnp.zeros_like(xh), jnp.broadcast_to(y, (LANES, half))]
        return jnp.concatenate(wide, axis=0)

    own = columns(own_ref, parity)
    other = columns(other_ref, 1 - parity)
    first = jnp.where(parity == 0, own, other)
    second = jnp.where(parity == 0, other, own)
    for c, ref in enumerate((first_ref, second_ref, third_ref)):
        at = slice(c * LANES, c * LANES + LANES)
        ref[pl.ds(0, half, 2), :] = first[at].T
        ref[pl.ds(1, half, 2), :] = second[at].T
    aug_ref[:, 0:LANES] = first_ref[...].astype(BF16)
    aug_ref[:, LANES : 2 * LANES] = second_ref[...].astype(BF16)
    y = third_ref[...]
    yh = y.astype(BF16).astype(F32)
    lane = lax.broadcasted_iota(I32, y.shape, 1)
    y_ref[...] = jnp.where(lane < LANES // 2, yh, y - yh).astype(BF16)
    sums = [jnp.zeros((SUBLANES, LANES), F32) for _ in range(2 * half // LANES)]
    for a, c in reversed(list(enumerate(coming))):
        c.wait()
        f = factor_block(f_ref, a, step)
        add_alpha(sums, f, two_parts(f), y_ref)
    for c, part in enumerate(sums):
        alpha_ref[:, c * LANES : c * LANES + LANES] = part


def factor_kernel(own_f_hbm, other_f_ref, y_ref, own_alpha_ref, fh_ref, fl_ref, alpha_ref, own_f_ref, sems, *, step):
    coming = factor_copies(own_f_hbm, own_f_ref, sems, step)
    for c in coming[::-1]:
        c.start()
    sums = [own_alpha_ref[:, c : c + LANES] for c in range(0, y_ref.shape[0], LANES)]
    for which, f_ref in ((1, other_f_ref), (0, own_f_ref)):
        rows = slice(step * which, step * which + step)
        for a, c in reversed(list(enumerate(coming))):
            if which == 0:
                c.wait()
            f = factor_block(f_ref, a, step)
            parts = two_parts(f)
            at = slice(first_column(a, step), first_column(a + 1, step))
            fh_ref[rows, at], fl_ref[rows, at] = parts
            if which == 1:
                add_alpha(sums, f, parts, y_ref)
    for c, part in enumerate(sums):
        alpha_ref[:, c * LANES : c * LANES + LANES] = jnp.broadcast_to(jnp.sum(part, axis=0, keepdims=True), (SUBLANES, LANES))


def expert_kernel(aug_ref, fh_ref, fl_ref, alpha_ref, slots_ref, mine_ref, theirs_ref, out_ref, kh_ref, kl_ref, *, scale, step):
    _, _, parity = place()
    points = aug_ref.shape[0]
    peers = slots_ref.shape[1]
    slots = slots_ref.shape[0] // 2
    part, width = mine_ref.shape
    features, block = 2 * part, width // slots
    mine, theirs = mine_ref[...], theirs_ref[...]
    t = jnp.concatenate([jnp.where(parity == 0, mine, theirs), jnp.where(parity == 0, theirs, mine)], axis=0)
    th, tm, tl = three_parts(t)
    square = -scale * jnp.sum(t * t, axis=0, keepdims=True)
    sh, sm, sl = three_parts(square)
    row = lax.broadcasted_iota(I32, (features, width), 0)
    last = jnp.where(row == 3, sh, jnp.where(row == 4, sm, jnp.where(row == 5, sl, 0.0)))
    last = jnp.where(row < 3, 1.0, last)
    taug = jnp.concatenate([th, tm, th, tm, tl, th, last, jnp.zeros_like(th)], axis=0).astype(BF16)
    quad = jnp.zeros((1, width), F32)
    mean = jnp.zeros((1, width), F32)
    for a in range(points // step):
        at = slice(a * step, a * step + step)
        k = jnp.exp2(jnp.dot(aug_ref[at, :], taug, preferred_element_type=F32))
        kh, kl = two_parts(k)
        kh_ref[at, :] = kh
        kl_ref[at, :] = kl
        alpha = jnp.concatenate(
            [
                jnp.broadcast_to(alpha_ref[0:1, c : c + LANES], (LANES, LANES)).T
                for c in range(a * step, a * step + step, LANES)
            ],
            axis=0,
        )
        mean = mean + jnp.sum(k * jnp.concatenate([alpha] * slots, axis=1), axis=0, keepdims=True)
    for a in range(points // step):
        reach = step * (a + 1)
        at = slice(first_column(a, step // 2), first_column(a, step // 2) + reach)
        solved = jnp.dot(fh_ref[:, at], kh_ref[0:reach, :], preferred_element_type=F32)
        solved = solved + jnp.dot(fl_ref[:, at], kh_ref[0:reach, :], preferred_element_type=F32)
        solved = solved + jnp.dot(fh_ref[:, at], kl_ref[0:reach, :], preferred_element_type=F32)
        quad = quad + jnp.sum(solved * solved, axis=0, keepdims=True)
    variance = NOISE + jnp.maximum(SIGNAL - quad, 0.0)
    gap = 0.5 * (math.log(SIGNAL + NOISE) - jnp.log(variance))
    weight = gap / variance
    both = jnp.concatenate([weight * mean, weight], axis=0)
    for r in range(peers):
        total = both[:, 0:block] * slots_ref[parity, r : r + 1]
        for m in range(1, slots):
            total = total + both[:, m * block : m * block + block] * slots_ref[2 * m + parity, r : r + 1]
        out_ref[r] = total


def owner_kernel(wanted_ref, parts_ref, out_ref):
    peers, _, _ = parts_ref.shape
    blocks = wanted_ref.shape[0]
    num, wgt = [], []
    for b in range(blocks):
        total = parts_ref[0] * wanted_ref[b, 0:1]
        for r in range(1, peers):
            total = total + parts_ref[r] * wanted_ref[b, r : r + 1]
        num.append(total[0:1])
        wgt.append(total[1:2])
    tile = jnp.concatenate(num + wgt, axis=0)
    for j in range(out_ref.shape[0]):
        out_ref[j] = tile


def final_kernel(parts_ref, mean_ref, var_ref):
    parts = [parts_ref[j] for j in range(parts_ref.shape[0])]
    while len(parts) > 1:
        parts = [parts[i] + parts[i + 1] for i in range(0, len(parts), 2)]
    total = parts[0]
    blocks = mean_ref.shape[0]
    precision = 1.0 / (SIGNAL + NOISE) + total[blocks:]
    mean_ref[...] = total[0:blocks] / precision
    var_ref[...] = 1.0 / precision


def hbm(x):
    return pltpu.with_memory_space_constraint(x, pltpu.HBM)


def vmem(x):
    return pltpu.with_memory_space_constraint(x, pltpu.VMEM)


def on_device(train_points, targets, inverse_factor, counts, membership, test_points):
    cols = lax.axis_size("col")
    rows = lax.axis_size("row")
    slots = min(8, rows) // 2
    blocks_own, features, block = test_points.shape
    half = train_points.shape[2]
    points = 2 * half
    scale = math.log2(math.e) / features
    swap = [(i, i ^ 1) for i in range(cols)]
    step = 128
    in_hbm = pl.BlockSpec(memory_space=pltpu.HBM)
    in_vmem = pl.BlockSpec(memory_space=pltpu.VMEM)
    held = features + SUBLANES

    outgoing, packed, wanted, table, valid = pl.pallas_call(
        send_kernel,
        out_shape=(
            pltpu.HBM((rows, features // 2, block), F32),
            pltpu.VMEM((held, half), F32),
            pltpu.VMEM((blocks_own, rows, LANES), F32),
            pltpu.VMEM((2 * slots, rows, LANES), F32),
            pltpu.VMEM((SUBLANES, LANES), F32),
        ),
        in_specs=[in_hbm] * 5,
        out_specs=(in_hbm,) + (in_vmem,) * 4,
        scratch_shapes=[
            pltpu.VMEM((rows, SUBLANES, membership.shape[2]), I32),
            pltpu.VMEM(counts.shape, I32),
            pltpu.VMEM((blocks_own, features // 2, block), F32),
            pltpu.VMEM((rows, features // 2, block), F32),
            pltpu.SemaphoreType.DMA((5 + rows // GROUP,)),
        ],
        compiler_params=pltpu.CompilerParams(vmem_limit_bytes=4 << 20),
        name="send",
    )(hbm(membership), hbm(counts), hbm(test_points), hbm(train_points), hbm(targets))
    tests = lax.all_to_all(outgoing, "row", split_axis=0, concat_axis=0, tiled=True)
    other = lax.ppermute(packed, "col", swap)
    other_factor = lax.ppermute(inverse_factor[0], "col", swap)

    chunks = half // step
    reach = first_column(chunks, step)
    held_f = [pltpu.VMEM((half, points), F32), pltpu.SemaphoreType.DMA((chunks,))]
    aug, y, own_alpha = pl.pallas_call(
        lambda *refs: points_kernel(*refs, features=features, factor=scale, step=step),
        out_shape=(
            pltpu.VMEM((points, 2 * LANES), BF16),
            pltpu.VMEM((points, LANES), BF16),
            pltpu.VMEM((SUBLANES, points), F32),
        ),
        in_specs=[in_vmem] * 3 + [in_hbm],
        out_specs=(in_vmem,) * 3,
        scratch_shapes=[pltpu.VMEM((points, LANES), F32)] * 3 + held_f,
        compiler_params=pltpu.CompilerParams(vmem_limit_bytes=16 << 20),
        name="points",
    )(vmem(valid), vmem(packed), vmem(other), hbm(inverse_factor))
    tests, aug = lax.optimization_barrier((tests, aug))
    mine, theirs = pl.pallas_call(
        pick_kernel,
        out_shape=(pltpu.VMEM((features // 2, slots * block), F32),) * 2,
        in_specs=[in_vmem] * 2,
        out_specs=(in_vmem,) * 2,
        compiler_params=pltpu.CompilerParams(vmem_limit_bytes=4 << 20),
        name="pick",
    )(vmem(table), vmem(tests))
    theirs = lax.ppermute(theirs, "col", swap)
    fh, fl, alpha = pl.pallas_call(
        lambda *refs: factor_kernel(*refs, step=step),
        out_shape=(
            pltpu.VMEM((2 * step, reach), BF16),
            pltpu.VMEM((2 * step, reach), BF16),
            pltpu.VMEM((SUBLANES, points), F32),
        ),
        in_specs=[in_hbm] + [in_vmem] * 3,
        out_specs=(in_vmem,) * 3,
        scratch_shapes=held_f,
        compiler_params=pltpu.CompilerParams(vmem_limit_bytes=12 << 20),
        name="factor",
    )(hbm(inverse_factor), vmem(other_factor), vmem(y), vmem(own_alpha))
    parts = pl.pallas_call(
        lambda *refs: expert_kernel(*refs, scale=scale, step=2 * step),
        out_shape=pltpu.VMEM((rows, 2, block), F32),
        in_specs=[in_vmem] * 7,
        out_specs=in_vmem,
        scratch_shapes=[pltpu.VMEM((points, slots * block), BF16)] * 2,
        compiler_params=pltpu.CompilerParams(vmem_limit_bytes=16 << 20),
        name="expert",
    )(*map(vmem, (aug, fh, fl, alpha, table, mine, theirs)))
    arrived = lax.all_to_all(parts, "row", split_axis=0, concat_axis=0, tiled=True)
    spread = pl.pallas_call(
        owner_kernel,
        out_shape=pltpu.VMEM((cols, 2 * blocks_own, block), F32),
        in_specs=[in_vmem] * 2,
        out_specs=in_vmem,
        compiler_params=pltpu.CompilerParams(vmem_limit_bytes=4 << 20),
        name="owner",
    )(vmem(wanted), vmem(arrived))
    shares = lax.all_to_all(spread, "col", split_axis=0, concat_axis=0, tiled=True)
    return pl.pallas_call(
        final_kernel,
        out_shape=(jax.ShapeDtypeStruct((blocks_own, block), F32),) * 2,
        in_specs=[in_vmem],
        out_specs=(in_vmem,) * 2,
        compiler_params=pltpu.CompilerParams(vmem_limit_bytes=4 << 20),
        name="final",
    )(vmem(shares))


def solution(mesh):
    in_specs = (
        P("row", None, "col"),
        P("row", "col"),
        P("row", "col", None),
        P("row", None),
        P(),
        P("row", None, None),
    )
    out_specs = (P("row", None), P("row", None))

    return jax.shard_map(on_device, mesh=mesh, in_specs=in_specs, out_specs=out_specs, check_vma=False)
```
